32 devices in a mesh: strip: 8 (over z, x), col: 4 (over y, core).
Axes of the slice: x: 2, y: 2, z: 4, core: 2. Of those that a mesh axis runs over, the one named last changes fastest.
Arguments:
- positions: float32 [3, 64, 1024], P(None, 'strip', 'col'), may hold values from -1.8 to 1.8
- target: float32 [3, 64, 1024], P(None, 'strip', 'col'), may hold values from -1.8 to 1.8
- inertia: float32 [64, 1024], P('strip', 'col'), may hold values from 1 to 4
- stiffness: float32 [3, 64, 1024], P(None, 'strip', 'col'), may hold values from 0.5 to 2
- pin_columns: int32 [64], replicated, may hold values from 0 to 1023
- inverses: bfloat16 [32, 512, 512], P('strip'), may hold values from -0.05 to 0.55
Outputs:
- displaced: float32 [3, 64, 1024], P(None, 'strip', 'col')
The draws below stay inside these ranges and needn't reach their ends.
Inputs may be any that keep to these rules, and one draw needn't show every extreme that they name: `pin_columns`: a column may appear more than once.
All inputs are finite; a program needn't handle non-finite values.
Results may differ from the reference program's by a relative error of at most 0.0003.
Values sent between devices are 32-bit elements; how exact they have to be, the bound alone decides.
A program may use at most 128 MiB of HBM per device.

```python
import math
import jax
import jax.numpy as jnp
from jax import lax

COL_DEV = 256
SROWS = 2
ITERS = 2
PINS = 64
NR = 64
NC = 1024
STRIPS = 32
N_COL = 4


def spring_field(key):
    keyed = jax.random.fold_in(key, 999983)
    field = jnp.exp(jax.random.uniform(keyed, (3, NR, NC), jnp.float32, math.log(0.5), math.log(2.0)))
    field = jnp.clip(field, 0.5, 2.0)
    carry_key = jax.random.fold_in(key, 999979)
    carry_rows = jax.random.uniform(carry_key, (NR // SROWS, NC), jnp.float32, 1.98, 2.0)
    return field.at[1, SROWS - 1::SROWS, :].set(carry_rows)


def draw_stiffness(key, part):
    return spring_field(key)


def draw_inverses(key, part):
    block_size = SROWS * COL_DEV
    strip_gain = 0.985
    carry_weights = spring_field(key)[1, SROWS - 1::SROWS, :]
    weight_means = jnp.mean(carry_weights, axis=1)
    places = jnp.arange(COL_DEV, dtype=jnp.float32)
    kernel = jnp.exp(-jnp.abs(places[:, None] - places[None, :]) / 8.0)
    kernel = kernel / jnp.sum(kernel, axis=1, keepdims=True)
    beside = jnp.eye(SROWS, k=1, dtype=jnp.float32) + jnp.eye(SROWS, k=-1, dtype=jnp.float32)
    own = 0.08 * jnp.eye(SROWS, dtype=jnp.float32)
    own_part = jnp.kron(own, kernel)
    beside_part = jnp.kron(beside, jnp.eye(COL_DEV, dtype=jnp.float32))

    def one_block(number):
        keyed = jax.random.fold_in(key, number)
        key_diag, key_jitter = jax.random.split(keyed)
        carried = strip_gain / weight_means[number]
        structure = own_part + carried * beside_part
        diagonal = jax.random.uniform(key_diag, (block_size,), jnp.float32, 0.05, 0.1)
        jitter = jnp.clip(jax.random.normal(key_jitter, (block_size, block_size), jnp.float32), -4.0, 4.0)
        jitter = jitter * (0.05 / block_size ** 0.5)
        return (structure + jnp.diag(diagonal) + jitter).astype(jnp.bfloat16)
    return lax.map(one_block, jnp.arange(STRIPS))


def place_ends(values, own_key, least, largest):
    longest = values.shape.index(max(values.shape))
    spots = []
    for shift in (0, 1):
        where = [jax.random.randint(jax.random.fold_in(own_key, axis), (), 0, length) for axis, length in enumerate(values.shape)]
        where[longest] = (where[longest] + shift) % values.shape[longest]
        spots.append(tuple(where))
    return values.at[spots[0]].set(least).at[spots[1]].set(largest)


def shard_levels(key, dims, cuts, smallest, high):
    loudness = 1.0
    for dim, parts in cuts:
        draws = jax.random.uniform(jax.random.fold_in(jax.random.fold_in(key, 6), dim), (parts,), jnp.float32, smallest / len(cuts), high / len(cuts))
        loudness = loudness * jnp.repeat(jnp.exp(draws), dims[dim] // parts).reshape((-1,) + (1,) * (len(dims) - 1 - dim))
    return loudness


def centred(key, extent, width, bound, cuts=(), kind=jnp.bfloat16):
    values = jax.random.normal(key, extent, jnp.float32) * width
    if len(cuts) > 0:
        values = shard_levels(key, extent, cuts, -0.22, 0.18) * values
    return jnp.clip(values, min=-bound, max=bound).astype(kind)


def setup_inputs(seed: int = 0) -> dict:
    seeds = jax.random.split(jax.random.key(seed), 7)
    positions = centred(seeds[0], (3, NR, NC), 0.3, 1.8, ((1, 8), (2, 4)), jnp.float32)
    target = centred(seeds[1], (3, NR, NC), 0.3, 1.8, ((1, 8), (2, 4)), jnp.float32)
    inertia = jnp.clip(jnp.exp(math.log(4.0) - 1.3862944 * jax.random.uniform(seeds[2], (NR, NC), jnp.float32) ** shard_levels(seeds[2], (NR, NC), ((0, 8), (1, 4)), -0.2, 0.2)), 1.0, 4.0)
    stiffness = draw_stiffness(jax.random.fold_in(seeds[6], 71), 0)
    pin_columns = place_ends(jax.random.randint(seeds[4], (PINS,), 0, NC), jax.random.fold_in(seeds[4], 1), 0, NC - 1).astype(jnp.int32)
    inverses = draw_inverses(jax.random.fold_in(seeds[6], 71), 0)
    return {"positions": positions, "target": target, "inertia": inertia, "stiffness": stiffness, "pin_columns": pin_columns, "inverses": inverses}


pin_stiffness = 20.0
highest = lax.Precision.HIGHEST

def times_transposed(rows_in, matrix):
    return lax.dot_general(rows_in, matrix, (((rows_in.ndim - 1,), (1,)), ((), ())), precision=highest, preferred_element_type=jnp.float32)

def axis_vector(offset, direction):
    entries = [0.0, 0.0, 0.0]
    entries[direction] = float(offset)
    return jnp.array(entries, jnp.float32).reshape(3, 1, 1)

def edge_force(top_side, low_side, weight, rest_vec, rest_len):
    spacing = rest_vec + low_side - top_side
    length = jnp.sqrt(lax.optimization_barrier(jnp.sum(spacing * spacing, axis=0, keepdims=True)))
    projected = rest_len * spacing / jnp.maximum(length, 0.5 * rest_len)
    return weight[None] * (projected - rest_vec)

def spring_forces(displaced, stiffness):
    summed = jnp.zeros_like(displaced)
    for offset, channel in ((1, 0), (2, 2)):
        pulling = edge_force(displaced[:, :, :-offset], displaced[:, :, offset:], stiffness[channel][:, :-offset], axis_vector(offset, 0), float(offset))
        summed = summed.at[:, :, :-offset].add(-pulling)
        summed = summed.at[:, :, offset:].add(pulling)
    pulling = edge_force(displaced[:, :-1, :], displaced[:, 1:, :], stiffness[1][:-1, :], axis_vector(1, 1), 1.0)
    summed = summed.at[:, :-1, :].add(-pulling)
    return summed.at[:, 1:, :].add(pulling)

def block_coupling(displaced, stiffness):
    coupled = jnp.zeros_like(displaced)
    for offset, channel in ((1, 0), (2, 2)):
        left_cols = jnp.arange(NC - offset, dtype=jnp.int32)
        crossing = (left_cols + offset) // COL_DEV != left_cols // COL_DEV
        cross_weight = jnp.where(crossing[None, :], stiffness[channel][:, :-offset], 0.0)
        coupled = coupled.at[:, :, :-offset].add(cross_weight[None] * displaced[:, :, offset:])
        coupled = coupled.at[:, :, offset:].add(cross_weight[None] * displaced[:, :, :-offset])
    row_ids = jnp.arange(NR - 1, dtype=jnp.int32)
    down_weight = jnp.where((row_ids % SROWS == SROWS - 1)[:, None], stiffness[1][:-1], 0.0)
    return coupled.at[:, :-1, :].add(down_weight[None] * displaced[:, 1:, :])

def gauss_seidel(rhs_field, stiffness, inverses):
    last_start = (SROWS - 1) * COL_DEV
    rhs_blocks = rhs_field.reshape(3, STRIPS, SROWS, N_COL, COL_DEV).transpose(1, 3, 0, 2, 4)
    rhs_blocks = rhs_blocks.reshape(STRIPS, N_COL, 3, SROWS * COL_DEV)
    weights_last = stiffness[1][SROWS - 1::SROWS].at[-1].set(0.0).reshape(STRIPS, N_COL, 1, COL_DEV)

    def advance(carried, inputs):
        rhs_strip, inverse, weight_row = inputs
        placed = jnp.pad(carried, ((0, 0), (0, 0), (0, last_start)))
        solved = times_transposed(rhs_strip + placed, inverse.astype(jnp.float32))
        return (weight_row * solved[:, :, last_start:], solved)
    start = jnp.zeros((N_COL, 3, COL_DEV), jnp.float32)
    unused, solved_all = lax.scan(advance, start, (rhs_blocks, inverses, weights_last))
    solved_all = solved_all.reshape(STRIPS, N_COL, 3, SROWS, COL_DEV).transpose(2, 0, 3, 1, 4)
    return solved_all.reshape(3, NR, NC)

def reference(positions, target, inertia, stiffness, pin_columns, inverses):
    pinned = jnp.any(pin_columns[:, None] == jnp.arange(NC, dtype=jnp.int32)[None, :], axis=0)
    pinned_row = jnp.where(pinned[None, :], positions[:, 0, :], 0.0)
    anchor = jnp.zeros_like(positions).at[:, 0, :].set(pinned_row)
    inertial = inertia[None] * target + pin_stiffness * anchor
    displaced = positions
    for sweep_number in range(ITERS):
        rhs_field = inertial + spring_forces(displaced, stiffness) + block_coupling(displaced, stiffness)
        displaced = gauss_seidel(rhs_field, stiffness, inverses)
    return displaced
```

```python
import functools

import jax
import jax.numpy as jnp
from jax import lax
from jax.experimental import pallas as pl
from jax.experimental.pallas import tpu as pltpu
from jax.sharding import PartitionSpec as P

ITERS = 2

pin_stiffness = 20.0
SUB = 8
LANES = 128
MESH = pl.DeviceIdType.MESH
f32 = jnp.float32
bf16 = jnp.bfloat16

TO_RIGHT, TO_LEFT, UP, DOWN = range(4)


def split(v):
    high = v.astype(bf16).astype(f32)
    return jnp.concatenate([high, v - high], axis=0).astype(bf16)


def folded(product):
    half = product.shape[0] // 2
    return product[:half] + product[half:]


def times_transposed(parts, matrix):
    product = lax.dot_general(
        parts, matrix, (((1,), (1,)), ((), ())), preferred_element_type=f32
    )
    return folded(product)


def times_pair(parts, high, low):
    product = jnp.dot(parts, high, preferred_element_type=f32) + jnp.dot(
        parts, low, preferred_element_type=f32
    )
    return folded(product)


def stretch(squared, rest_len):
    return rest_len * jnp.minimum(lax.rsqrt(squared), 2.0 / rest_len)


def kernel(
    n_strip, n_col,
    pins, pos, tgt, inertia, stf, inv,
    out,
    mats, high, low, disp, halo, halo_w, send_row, recv_row, edge_w, cross_w,
    inv_sem, side_send, side_recv, w_send, w_recv, row_send, row_recv,
):
    rows, cols = pos.shape[1], pos.shape[2]
    strips = inv.shape[0]
    srows = rows // strips
    block = srows * cols
    last_start = block - cols
    me_s, me_c = lax.axis_index("strip"), lax.axis_index("col")
    not_top, not_bottom = me_s > 0, me_s < n_strip - 1
    not_left, not_right = me_c > 0, me_c < n_col - 1

    loads = [pltpu.make_async_copy(inv.at[k], mats.at[k], inv_sem.at[k]) for k in range(strips)]
    for load in loads:
        load.start()

    barrier = pltpu.get_barrier_semaphore()
    sides = (
        (not_top, (me_s - 1, me_c)),
        (not_bottom, (me_s + 1, me_c)),
        (not_left, (me_s, me_c - 1)),
        (not_right, (me_s, me_c + 1)),
    )
    for there, device in sides:
        @pl.when(there)
        def _():
            pl.semaphore_signal(barrier, inc=1, device_id=device, device_id_type=MESH)

    def side_copies(sweep):
        source = pos if sweep == 0 else disp
        right = pltpu.make_async_remote_copy(
            src_ref=source.at[:, :, pl.ds(cols - LANES, LANES)], dst_ref=halo.at[sweep, 0],
            send_sem=side_send.at[sweep, 0], recv_sem=side_recv.at[sweep, 0],
            device_id=(me_s, me_c + 1), device_id_type=MESH)
        left = pltpu.make_async_remote_copy(
            src_ref=source.at[:, :, pl.ds(0, LANES)], dst_ref=halo.at[sweep, 1],
            send_sem=side_send.at[sweep, 1], recv_sem=side_recv.at[sweep, 1],
            device_id=(me_s, me_c - 1), device_id_type=MESH)
        return right, left

    weights_right = pltpu.make_async_remote_copy(
        src_ref=stf.at[:, :, pl.ds(cols - LANES, LANES)], dst_ref=halo_w,
        send_sem=w_send, recv_sem=w_recv,
        device_id=(me_s, me_c + 1), device_id_type=MESH)

    def row_copy(number, step):
        return pltpu.make_async_remote_copy(
            src_ref=send_row.at[number], dst_ref=recv_row.at[number],
            send_sem=row_send.at[number], recv_sem=row_recv.at[number],
            device_id=(me_s + step, me_c), device_id_type=MESH)

    ups = [row_copy(t, -1) for t in range(ITERS)]
    downs = [row_copy(ITERS + t, 1) for t in range(ITERS + 1)]
    side = [side_copies(t) for t in range(ITERS)]

    row_of = lax.broadcasted_iota(jnp.int32, (SUB, cols), 0)
    field_row = lax.broadcasted_iota(jnp.int32, (rows, cols), 0)

    def compact(parts):
        total = jnp.zeros((SUB, cols), f32)
        for place, part in enumerate(parts):
            total = jnp.where(row_of == place, jnp.broadcast_to(part, (SUB, cols)), total)
        return total

    send_row[0] = compact([pos[c, 0:1] for c in range(3)])
    send_row[ITERS] = compact(
        [pos[c, rows - 1:rows] for c in range(3)] + [stf[1, rows - 1:rows]])

    @pl.when(jnp.logical_not(not_top))
    def _():
        for t in range(ITERS + 1):
            recv_row[ITERS + t] = jnp.zeros((SUB, cols), f32)

    @pl.when(jnp.logical_not(not_bottom))
    def _():
        for t in range(ITERS):
            recv_row[t] = jnp.zeros((SUB, cols), f32)

    @pl.when(jnp.logical_not(not_left))
    def _():
        halo_w[...] = jnp.zeros_like(halo_w)
        for t in range(ITERS):
            halo[t, 0] = jnp.zeros((3, rows, LANES), f32)

    @pl.when(jnp.logical_not(not_right))
    def _():
        for t in range(ITERS):
            halo[t, 1] = jnp.zeros((3, rows, LANES), f32)

    neighbours = sum(there.astype(jnp.int32) for there, _ in sides)
    pl.semaphore_wait(barrier, neighbours)

    @pl.when(not_right)
    def _():
        side[0][0].start()
        weights_right.start()

    @pl.when(not_left)
    def _():
        side[0][1].start()

    @pl.when(not_bottom)
    def _():
        downs[0].start()

    @pl.when(not_top)
    def _():
        ups[0].start()

    own_cols = lax.broadcasted_iota(jnp.int32, (1, cols), 1) + me_c * cols
    pinned = jnp.zeros((1, cols), jnp.int32)
    for number in range(pins.shape[0]):
        pinned = pinned | (own_cols == pins[number]).astype(jnp.int32)
    pinned = jnp.broadcast_to(pinned, (rows, cols)) * (field_row == 0) * jnp.where(not_top, 0, 1)
    inertial = [
        inertia[...] * tgt[c] + jnp.where(pinned > 0, pin_stiffness * pos[c], 0.0)
        for c in range(3)
    ]

    w_strip = [stf[1, srows * (k + 1) - 1:srows * (k + 1)] for k in range(strips)]
    eye = (
        lax.broadcasted_iota(jnp.int32, (cols, cols), 0)
        == lax.broadcasted_iota(jnp.int32, (cols, cols), 1)
    ).astype(f32).astype(bf16)
    product = None
    for k in range(strips):
        loads[k].wait()
        matrix = mats[k, last_start:, :cols]
        if k == 0:
            product = lax.dot_general(
                eye, matrix, (((1,), (1,)), ((), ())), preferred_element_type=f32)
        else:
            product = times_transposed(
                jnp.concatenate([high[k - 1], low[k - 1]], axis=0), matrix)
        if k < strips - 1:
            product = product * w_strip[k]
        upper = product.astype(bf16)
        high[k] = upper
        low[k] = (product - upper.astype(f32)).astype(bf16)

    wide = cols + 2 * LANES
    wide_lane = lax.broadcasted_iota(jnp.int32, (rows, wide), 1) - LANES
    wide_cols = wide_lane + me_c * cols
    grid_cols = n_col * cols
    vertical = jnp.where(field_row < rows - 1, stf[1], 0.0)
    is_last = field_row % srows == srows - 1
    w_down = jnp.where(is_last, vertical, 0.0)
    w_bottom = jnp.where(not_bottom, stf[1, rows - 1:rows], 0.0)
    rest_row = jnp.where(row_of == 1, 1.0, 0.0)

    def early_rhs(u, left, right, above, w_above):
        field = [jnp.concatenate([left[c], u[c], right[c]], axis=1) for c in range(3)]
        total = [jnp.zeros((rows, wide), f32)] * 3
        for number, offset in enumerate((1, 2)):
            ahead = [pltpu.roll(field[c], wide - offset, axis=1) for c in range(3)]
            gap = [ahead[c] - field[c] for c in range(3)]
            gap[0] = gap[0] + float(offset)
            scale = stretch(gap[0] * gap[0] + gap[1] * gap[1] + gap[2] * gap[2], float(offset))
            weight, cross = edge_w[number], cross_w[number]
            for c in range(3):
                moved = scale * gap[c]
                if c == 0:
                    moved = moved - float(offset)
                pull = weight * moved
                at_a = cross * ahead[c] - pull
                at_b = cross * field[c] + pull
                total[c] = total[c] + at_a + pltpu.roll(at_b, offset, axis=1)
        below = [pltpu.roll(u[c], rows - 1, axis=0) for c in range(3)]
        before = [
            jnp.where(field_row == 0, jnp.broadcast_to(above[c:c + 1], (rows, cols)),
                      pltpu.roll(u[c], 1, axis=0))
            for c in range(3)
        ]
        w_before = jnp.where(
            field_row == 0, jnp.broadcast_to(w_above, (rows, cols)),
            pltpu.roll(stf[1], 1, axis=0))
        gap = [below[c] - u[c] for c in range(3)]
        gap[1] = gap[1] + 1.0
        scale = stretch(gap[0] * gap[0] + gap[1] * gap[1] + gap[2] * gap[2], 1.0)
        back = [u[c] - before[c] for c in range(3)]
        back[1] = back[1] + 1.0
        back_scale = stretch(back[0] * back[0] + back[1] * back[1] + back[2] * back[2], 1.0)
        result = []
        for c in range(3):
            rest = 1.0 if c == 1 else 0.0
            value = inertial[c] + total[c][:, LANES:LANES + cols]
            value = value - vertical * (scale * gap[c] - rest) + w_down * below[c]
            result.append(value + w_before * (back_scale * back[c] - rest))
        return result

    def late_rhs(last_rows, below):
        gap = below - last_rows + rest_row
        scale = stretch(jnp.sum(gap * gap, axis=0, keepdims=True), 1.0)
        return w_bottom * (below - scale * gap + rest_row)

    def strip_vector(rhs, k):
        return [
            compact([rhs[c][srows * k + i:srows * k + i + 1] for c in range(3)])
            for i in range(srows)
        ]

    def receive(copy, there):
        @pl.when(there)
        def _():
            copy.wait_recv()

    def send(copy, there):
        @pl.when(there)
        def _():
            copy.start()

    @pl.when(not_left)
    def _():
        weights_right.wait_recv()

    for number, (offset, channel) in enumerate(((1, 0), (2, 2))):
        weight = jnp.concatenate(
            [halo_w[channel], stf[channel], jnp.zeros((rows, LANES), f32)], axis=1)
        inside = (wide_cols >= 0) & (wide_cols + offset <= grid_cols - 1)
        weight = jnp.where(inside, weight, 0.0)
        crossing = ((wide_lane < 0) & (wide_lane + offset >= 0)) | (
            (wide_lane < cols) & (wide_lane + offset >= cols))
        edge_w[number] = weight
        cross_w[number] = jnp.where(crossing, weight, 0.0)

    receive(downs[0], not_top)
    above = recv_row[ITERS]
    w_above = jnp.where(not_top, above[3:4], 0.0)
    current = [pos[c] for c in range(3)]
    last_rows = compact([pos[c, rows - 1:rows] for c in range(3)])

    for sweep in range(ITERS):
        receive(side[sweep][0], not_left)
        receive(side[sweep][1], not_right)
        rhs = early_rhs(
            current, [halo[sweep, 0, c] for c in range(3)], [halo[sweep, 1, c] for c in range(3)],
            above, w_above)
        vectors = [strip_vector(rhs, k) for k in range(strips)]
        if sweep == 0:
            receive(ups[sweep], not_bottom)
            vectors[-1][-1] = vectors[-1][-1] + late_rhs(last_rows, recv_row[sweep])
        base, offsets = [], []
        for k in range(strips):
            parts = split(jnp.concatenate(vectors[k], axis=1))
            base.append(times_transposed(parts, mats[k]))
        carried = None
        for k in range(strips):
            if k == 0:
                carried = base[k][:, last_start:]
            else:
                carried = base[k][:, last_start:] + times_transposed(
                    split(carried), mats[k, last_start:, :cols])
            if k < strips - 1:
                carried = carried * w_strip[k]
            offsets.append(carried)
        if sweep > 0:
            receive(ups[sweep], not_bottom)
            late = split(late_rhs(last_rows, recv_row[sweep]))
            change = times_transposed(late, mats[strips - 1, :, last_start:])
            base[-1] = base[-1] + change
            offsets[-1] = offsets[-1] + change[:, last_start:]

        receive(downs[sweep + 1], not_top)
        above = recv_row[ITERS + sweep + 1]
        entering = split(above * w_above)
        last_rows = offsets[-1] + times_pair(entering, high[strips - 1], low[strips - 1])
        send_row[ITERS + sweep + 1] = last_rows
        send(downs[sweep + 1], not_bottom)
        solved = [base[0] + times_transposed(entering, mats[0, :, :cols])]
        if sweep < ITERS - 1:
            send_row[sweep + 1] = solved[0][:, :cols]
            send(ups[sweep + 1], not_top)
        for k in range(1, strips):
            carried = offsets[k - 1] + times_pair(entering, high[k - 1], low[k - 1])
            solved.append(base[k] + times_transposed(split(carried), mats[k, :, :cols]))
        current = []
        for c in range(3):
            field = jnp.zeros((rows, cols), f32)
            for k in range(strips):
                for i in range(srows):
                    row = solved[k][c:c + 1, i * cols:(i + 1) * cols]
                    field = jnp.where(
                        field_row == srows * k + i, jnp.broadcast_to(row, (rows, cols)), field)
            current.append(field)
            if sweep < ITERS - 1:
                disp[c] = field
            else:
                out[c] = field
        if sweep < ITERS - 1:
            send(side[sweep + 1][0], not_right)
            send(side[sweep + 1][1], not_left)

    def sent(copy, there):
        @pl.when(there)
        def _():
            copy.wait_send()

    sent(weights_right, not_right)
    for right, left in side:
        sent(right, not_right)
        sent(left, not_left)
    for copy in ups:
        sent(copy, not_top)
    for copy in downs:
        sent(copy, not_bottom)


def shards(n_strip, n_col, positions, target, inertia, stiffness, pin_columns, inverses):
    rows, cols = positions.shape[1:]
    strips, block, _ = inverses.shape
    vmem = pl.BlockSpec(memory_space=pltpu.VMEM)
    dma = pltpu.SemaphoreType.DMA
    return pl.pallas_call(
        functools.partial(kernel, n_strip, n_col),
        out_shape=jax.ShapeDtypeStruct(positions.shape, f32),
        in_specs=[pl.BlockSpec(memory_space=pltpu.SMEM)] + [vmem] * 4
        + [pl.BlockSpec(memory_space=pl.ANY)],
        out_specs=vmem,
        scratch_shapes=[
            pltpu.VMEM(inverses.shape, bf16),
            pltpu.VMEM((strips, cols, cols), bf16),
            pltpu.VMEM((strips, cols, cols), bf16),
            pltpu.VMEM(positions.shape, f32),
            pltpu.VMEM((ITERS, 2, 3, rows, LANES), f32),
            pltpu.VMEM((3, rows, LANES), f32),
            pltpu.VMEM((2 * ITERS + 1, SUB, cols), f32),
            pltpu.VMEM((2 * ITERS + 1, SUB, cols), f32),
            pltpu.VMEM((2, rows, cols + 2 * LANES), f32),
            pltpu.VMEM((2, rows, cols + 2 * LANES), f32),
            dma((strips,)),
            dma((ITERS, 2)),
            dma((ITERS, 2)),
            dma,
            dma,
            dma((2 * ITERS + 1,)),
            dma((2 * ITERS + 1,)),
        ],
        compiler_params=pltpu.CompilerParams(
            collective_id=0, has_side_effects=True, vmem_limit_bytes=32 * 1024 * 1024),
    )(pin_columns, positions, target, inertia, stiffness, inverses)


def solution(mesh):
    in_specs = (
        P(None, "strip", "col"),
        P(None, "strip", "col"),
        P("strip", "col"),
        P(None, "strip", "col"),
        P(),
        P("strip", None, None),
    )
    out_specs = P(None, "strip", "col")
    run = functools.partial(shards, mesh.shape["strip"], mesh.shape["col"])
    return jax.shard_map(run, mesh=mesh, in_specs=in_specs, out_specs=out_specs, check_vma=False)
```

```python
import functools

import jax
import jax.numpy as jnp
from jax import lax
from jax.experimental import pallas as pl
from jax.experimental.pallas import tpu as pltpu
from jax.sharding import PartitionSpec as P

ITERS = 2

pin_stiffness = 20.0
SUB = 8
LANES = 128
MESH = pl.DeviceIdType.MESH
f32 = jnp.float32
bf16 = jnp.bfloat16


def split(v):
    high = v.astype(bf16).astype(f32)
    return jnp.concatenate([high, v - high], axis=0).astype(bf16)


def folded(product):
    half = product.shape[0] // 2
    return product[:half] + product[half:]


def times_transposed(parts, matrix):
    product = lax.dot_general(
        parts, matrix, (((1,), (1,)), ((), ())), preferred_element_type=f32
    )
    return folded(product)


def times_pair(parts, high, low):
    product = jnp.dot(parts, high, preferred_element_type=f32) + jnp.dot(
        parts, low, preferred_element_type=f32
    )
    return folded(product)


def stretch(squared, rest_len):
    return rest_len * jnp.minimum(lax.rsqrt(squared), 2.0 / rest_len)


def kernel(
    n_strip, n_col,
    pins_in, pos_in, tgt_in, inertia_in, stf_in, inv,
    out,
    pins, pos, tgt, inertia, stf,
    mats, high, low, disp, halo, halo_w, send_row, recv_row, edge_w, cross_w,
    map_send, map_recv, map_high, map_low, both_high, both_low, above_row,
    in_sem, inv_sem, side_send, side_recv, w_send, w_recv, row_send, row_recv, m_send, m_recv,
):
    rows, cols = pos.shape[1], pos.shape[2]
    strips = inv.shape[0]
    srows = rows // strips
    block = srows * cols
    last_start = block - cols
    me_s, me_c = lax.axis_index("strip"), lax.axis_index("col")
    not_top, not_bottom = me_s > 0, me_s < n_strip - 1
    not_left, not_right = me_c > 0, me_c < n_col - 1

    is_tail, is_lead = me_s % 2 == 1, me_s % 2 == 0
    tail_after = is_tail & (me_s + 2 < n_strip)
    tail_before = is_tail & (me_s >= 2)
    lead_before = is_lead & not_top
    mapped_lead = lead_before & not_bottom

    fetches = [
        pltpu.make_async_copy(source, target, in_sem.at[number])
        for number, (source, target) in enumerate((
            (pos_in, pos), (stf_in, stf), (pins_in, pins), (tgt_in, tgt), (inertia_in, inertia)))
    ]
    for fetch in fetches:
        fetch.start()
    loads = [pltpu.make_async_copy(inv.at[k], mats.at[k], inv_sem.at[k]) for k in range(strips)]
    for load in loads:
        load.start()

    barrier = pltpu.get_barrier_semaphore()
    sides = (
        (not_top, (me_s - 1, me_c)),
        (not_bottom, (me_s + 1, me_c)),
        (not_left, (me_s, me_c - 1)),
        (not_right, (me_s, me_c + 1)),
        (tail_before, (me_s - 2, me_c)),
        (tail_after, (me_s + 2, me_c)),
    )
    for there, device in sides:
        @pl.when(there)
        def _():
            pl.semaphore_signal(barrier, inc=1, device_id=device, device_id_type=MESH)

    def side_copies(sweep):
        source = pos if sweep == 0 else disp
        right = pltpu.make_async_remote_copy(
            src_ref=source.at[:, :, pl.ds(cols - LANES, LANES)], dst_ref=halo.at[sweep, 0],
            send_sem=side_send.at[sweep, 0], recv_sem=side_recv.at[sweep, 0],
            device_id=(me_s, me_c + 1), device_id_type=MESH)
        left = pltpu.make_async_remote_copy(
            src_ref=source.at[:, :, pl.ds(0, LANES)], dst_ref=halo.at[sweep, 1],
            send_sem=side_send.at[sweep, 1], recv_sem=side_recv.at[sweep, 1],
            device_id=(me_s, me_c - 1), device_id_type=MESH)
        return right, left

    weights_right = pltpu.make_async_remote_copy(
        src_ref=stf.at[:, :, pl.ds(cols - LANES, LANES)], dst_ref=halo_w,
        send_sem=w_send, recv_sem=w_recv,
        device_id=(me_s, me_c + 1), device_id_type=MESH)

    def row_copy(number, step):
        return pltpu.make_async_remote_copy(
            src_ref=send_row.at[number], dst_ref=recv_row.at[number],
            send_sem=row_send.at[number], recv_sem=row_recv.at[number],
            device_id=(me_s + step, me_c), device_id_type=MESH)

    ups = [row_copy(t, -1) for t in range(ITERS)]
    first_down = row_copy(ITERS, 1)
    base_row = ITERS + 1
    lead_out = [row_copy(base_row + t, 1) for t in range(ITERS)]
    tail_out = [row_copy(base_row + ITERS + t, 2) for t in range(ITERS)]
    next_out = [row_copy(base_row + 2 * ITERS + t, 1) for t in range(ITERS)]
    map_copy = pltpu.make_async_remote_copy(
        src_ref=map_send, dst_ref=map_recv, send_sem=m_send, recv_sem=m_recv,
        device_id=(me_s + 1, me_c), device_id_type=MESH)
    side = [side_copies(t) for t in range(ITERS)]

    row_of = lax.broadcasted_iota(jnp.int32, (SUB, cols), 0)
    field_row = lax.broadcasted_iota(jnp.int32, (rows, cols), 0)

    def compact(parts):
        total = jnp.zeros((SUB, cols), f32)
        for place, part in enumerate(parts):
            total = jnp.where(row_of == place, jnp.broadcast_to(part, (SUB, cols)), total)
        return total

    fetches[0].wait()
    fetches[1].wait()
    send_row[0] = compact([pos[c, 0:1] for c in range(3)])
    send_row[ITERS] = compact(
        [pos[c, rows - 1:rows] for c in range(3)] + [stf[1, rows - 1:rows]])

    @pl.when(jnp.logical_not(not_top))
    def _():
        recv_row[ITERS] = jnp.zeros((SUB, cols), f32)

    @pl.when(jnp.logical_not(not_bottom))
    def _():
        for t in range(ITERS):
            recv_row[t] = jnp.zeros((SUB, cols), f32)

    @pl.when(jnp.logical_not(not_left))
    def _():
        halo_w[...] = jnp.zeros_like(halo_w)
        for t in range(ITERS):
            halo[t, 0] = jnp.zeros((3, rows, LANES), f32)

    @pl.when(jnp.logical_not(not_right))
    def _():
        for t in range(ITERS):
            halo[t, 1] = jnp.zeros((3, rows, LANES), f32)

    for fetch in fetches[2:]:
        fetch.wait()
    own_cols = lax.broadcasted_iota(jnp.int32, (1, cols), 1) + me_c * cols
    pinned = jnp.zeros((1, cols), jnp.int32)
    for number in range(pins.shape[0]):
        pinned = pinned | (own_cols == pins[number]).astype(jnp.int32)
    pinned = jnp.broadcast_to(pinned, (rows, cols)) * (field_row == 0) * jnp.where(not_top, 0, 1)
    inertial = [
        inertia[...] * tgt[c] + jnp.where(pinned > 0, pin_stiffness * pos[c], 0.0)
        for c in range(3)
    ]

    neighbours = sum(there.astype(jnp.int32) for there, _ in sides)
    pl.semaphore_wait(barrier, neighbours)

    @pl.when(not_right)
    def _():
        side[0][0].start()
        weights_right.start()

    @pl.when(not_left)
    def _():
        side[0][1].start()

    @pl.when(not_bottom)
    def _():
        first_down.start()

    @pl.when(not_top)
    def _():
        ups[0].start()

    w_strip = [stf[1, srows * (k + 1) - 1:srows * (k + 1)] for k in range(strips)]
    eye = (
        lax.broadcasted_iota(jnp.int32, (cols, cols), 0)
        == lax.broadcasted_iota(jnp.int32, (cols, cols), 1)
    ).astype(f32).astype(bf16)
    product = None
    for k in range(strips):
        loads[k].wait()
        matrix = mats[k, last_start:, :cols]
        if k == 0:
            product = lax.dot_general(
                eye, matrix, (((1,), (1,)), ((), ())), preferred_element_type=f32)
        else:
            product = times_transposed(
                jnp.concatenate([high[k - 1], low[k - 1]], axis=0), matrix)
        if k < strips - 1:
            product = product * w_strip[k]
        else:
            map_send[...] = product

            @pl.when(mapped_lead)
            def _():
                map_copy.start()
        upper = product.astype(bf16)
        high[k] = upper
        low[k] = (product - upper.astype(f32)).astype(bf16)

    wide = cols + 2 * LANES
    wide_lane = lax.broadcasted_iota(jnp.int32, (rows, wide), 1) - LANES
    wide_cols = wide_lane + me_c * cols
    grid_cols = n_col * cols
    vertical = jnp.where(field_row < rows - 1, stf[1], 0.0)
    is_last = field_row % srows == srows - 1
    w_down = jnp.where(is_last, vertical, 0.0)
    w_bottom = jnp.where(not_bottom, stf[1, rows - 1:rows], 0.0)
    rest_row = jnp.where(row_of == 1, 1.0, 0.0)

    def early_rhs(u, left, right, above, w_above):
        field = [jnp.concatenate([left[c], u[c], right[c]], axis=1) for c in range(3)]
        total = [jnp.zeros((rows, wide), f32)] * 3
        for number, offset in enumerate((1, 2)):
            ahead = [pltpu.roll(field[c], wide - offset, axis=1) for c in range(3)]
            gap = [ahead[c] - field[c] for c in range(3)]
            gap[0] = gap[0] + float(offset)
            scale = stretch(gap[0] * gap[0] + gap[1] * gap[1] + gap[2] * gap[2], float(offset))
            weight, cross = edge_w[number], cross_w[number]
            for c in range(3):
                moved = scale * gap[c]
                if c == 0:
                    moved = moved - float(offset)
                pull = weight * moved
                at_a = cross * ahead[c] - pull
                at_b = cross * field[c] + pull
                total[c] = total[c] + at_a + pltpu.roll(at_b, offset, axis=1)
        below = [pltpu.roll(u[c], rows - 1, axis=0) for c in range(3)]
        before = [
            jnp.where(field_row == 0, jnp.broadcast_to(above[c:c + 1], (rows, cols)),
                      pltpu.roll(u[c], 1, axis=0))
            for c in range(3)
        ]
        w_before = jnp.where(
            field_row == 0, jnp.broadcast_to(w_above, (rows, cols)),
            pltpu.roll(stf[1], 1, axis=0))
        gap = [below[c] - u[c] for c in range(3)]
        gap[1] = gap[1] + 1.0
        scale = stretch(gap[0] * gap[0] + gap[1] * gap[1] + gap[2] * gap[2], 1.0)
        back = [u[c] - before[c] for c in range(3)]
        back[1] = back[1] + 1.0
        back_scale = stretch(back[0] * back[0] + back[1] * back[1] + back[2] * back[2], 1.0)
        result = []
        for c in range(3):
            rest = 1.0 if c == 1 else 0.0
            value = inertial[c] + total[c][:, LANES:LANES + cols]
            value = value - vertical * (scale * gap[c] - rest) + w_down * below[c]
            result.append(value + w_before * (back_scale * back[c] - rest))
        return result

    def late_rhs(last_rows, below):
        gap = below - last_rows + rest_row
        scale = stretch(jnp.sum(gap * gap, axis=0, keepdims=True), 1.0)
        return w_bottom * (below - scale * gap + rest_row)

    def strip_vector(rhs, k):
        return [
            compact([rhs[c][srows * k + i:srows * k + i + 1] for c in range(3)])
            for i in range(srows)
        ]

    def receive(copy, there):
        @pl.when(there)
        def _():
            copy.wait_recv()

    def send(copy, there):
        @pl.when(there)
        def _():
            copy.start()

    @pl.when(not_left)
    def _():
        weights_right.wait_recv()

    for number, (offset, channel) in enumerate(((1, 0), (2, 2))):
        weight = jnp.concatenate(
            [halo_w[channel], stf[channel], jnp.zeros((rows, LANES), f32)], axis=1)
        inside = (wide_cols >= 0) & (wide_cols + offset <= grid_cols - 1)
        weight = jnp.where(inside, weight, 0.0)
        crossing = ((wide_lane < 0) & (wide_lane + offset >= 0)) | (
            (wide_lane < cols) & (wide_lane + offset >= cols))
        edge_w[number] = weight
        cross_w[number] = jnp.where(crossing, weight, 0.0)

    receive(first_down, not_top)
    above = recv_row[ITERS]
    w_above = jnp.where(not_top, above[3:4], 0.0)
    current = [pos[c] for c in range(3)]
    last_rows = compact([pos[c, rows - 1:rows] for c in range(3)])

    for sweep in range(ITERS):
        receive(side[sweep][0], not_left)
        receive(side[sweep][1], not_right)
        rhs = early_rhs(
            current, [halo[sweep, 0, c] for c in range(3)], [halo[sweep, 1, c] for c in range(3)],
            above, w_above)
        vectors = [strip_vector(rhs, k) for k in range(strips)]
        if sweep == 0:
            receive(ups[sweep], not_bottom)
            vectors[-1][-1] = vectors[-1][-1] + late_rhs(last_rows, recv_row[sweep])
        base, offsets = [], []
        for k in range(strips):
            parts = split(jnp.concatenate(vectors[k], axis=1))
            base.append(times_transposed(parts, mats[k]))
        carried = None
        for k in range(strips):
            if k == 0:
                carried = base[k][:, last_start:]
            else:
                carried = base[k][:, last_start:] + times_transposed(
                    split(carried), mats[k, last_start:, :cols])
            if k < strips - 1:
                carried = carried * w_strip[k]
            offsets.append(carried)
        if sweep > 0:
            receive(ups[sweep], not_bottom)
            late = split(late_rhs(last_rows, recv_row[sweep]))
            change = times_transposed(late, mats[strips - 1, :, last_start:])
            base[-1] = base[-1] + change
            offsets[-1] = offsets[-1] + change[:, last_start:]

        send_row[base_row + sweep] = offsets[-1]
        send(lead_out[sweep], is_lead & not_bottom)

        def pass_on(tail_rows):
            send_row[base_row + ITERS + sweep] = tail_rows * w_bottom
            send_row[base_row + 2 * ITERS + sweep] = tail_rows
            send(tail_out[sweep], tail_after)
            send(next_out[sweep], is_tail & not_bottom)

        @pl.when(is_tail)
        def _():
            lead_out[sweep].wait_recv()
            lead_rows = recv_row[base_row + sweep]
            tail_rows = offsets[-1] + times_pair(
                split(lead_rows * w_above), high[strips - 1], low[strips - 1])

            @pl.when(jnp.logical_not(tail_before))
            def _():
                pass_on(tail_rows)
                above_row[...] = lead_rows

            @pl.when(tail_before)
            def _():
                if sweep == 0:
                    map_copy.wait_recv()
                    received = map_recv[...]
                    upper = received.astype(bf16)
                    map_high[...] = upper
                    map_low[...] = (received - upper.astype(f32)).astype(bf16)
                    both = times_pair(
                        split(received * w_above), high[strips - 1], low[strips - 1])
                    upper = both.astype(bf16)
                    both_high[...] = upper
                    both_low[...] = (both - upper.astype(f32)).astype(bf16)
                tail_out[sweep].wait_recv()
                entering = split(recv_row[base_row + ITERS + sweep])
                pass_on(tail_rows + times_pair(entering, both_high[...], both_low[...]))
                above_row[...] = lead_rows + times_pair(entering, map_high[...], map_low[...])

        @pl.when(lead_before)
        def _():
            next_out[sweep].wait_recv()
            above_row[...] = recv_row[base_row + 2 * ITERS + sweep]

        @pl.when(jnp.logical_not(not_top))
        def _():
            above_row[...] = jnp.zeros((SUB, cols), f32)

        above = above_row[...]
        entering = split(above * w_above)
        solved = [base[0] + times_transposed(entering, mats[0, :, :cols])]
        if sweep < ITERS - 1:
            send_row[sweep + 1] = solved[0][:, :cols]
            send(ups[sweep + 1], not_top)
        for k in range(1, strips):
            carried = offsets[k - 1] + times_pair(entering, high[k - 1], low[k - 1])
            solved.append(base[k] + times_transposed(split(carried), mats[k, :, :cols]))
        last_rows = solved[-1][:, last_start:]
        current = []
        for c in range(3):
            field = jnp.zeros((rows, cols), f32)
            for k in range(strips):
                for i in range(srows):
                    row = solved[k][c:c + 1, i * cols:(i + 1) * cols]
                    field = jnp.where(
                        field_row == srows * k + i, jnp.broadcast_to(row, (rows, cols)), field)
            current.append(field)
            if sweep < ITERS - 1:
                disp[c] = field
            else:
                out[c] = field
        if sweep < ITERS - 1:
            send(side[sweep + 1][0], not_right)
            send(side[sweep + 1][1], not_left)

    def sent(copy, there):
        @pl.when(there)
        def _():
            copy.wait_send()

    sent(weights_right, not_right)
    for right, left in side:
        sent(right, not_right)
        sent(left, not_left)
    for copy in ups:
        sent(copy, not_top)
    sent(first_down, not_bottom)
    sent(map_copy, mapped_lead)
    for t in range(ITERS):
        sent(lead_out[t], is_lead & not_bottom)
        sent(tail_out[t], tail_after)
        sent(next_out[t], is_tail & not_bottom)


def shards(n_strip, n_col, positions, target, inertia, stiffness, pin_columns, inverses):
    rows, cols = positions.shape[1:]
    strips, block, _ = inverses.shape
    messages = 4 * ITERS + 1
    dma = pltpu.SemaphoreType.DMA
    return pl.pallas_call(
        functools.partial(kernel, n_strip, n_col),
        out_shape=jax.ShapeDtypeStruct(positions.shape, f32),
        in_specs=[pl.BlockSpec(memory_space=pltpu.HBM)] * 6,
        out_specs=pl.BlockSpec(memory_space=pltpu.VMEM),
        scratch_shapes=[
            pltpu.SMEM(pin_columns.shape, jnp.int32),
            pltpu.VMEM(positions.shape, f32),
            pltpu.VMEM(target.shape, f32),
            pltpu.VMEM(inertia.shape, f32),
            pltpu.VMEM(stiffness.shape, f32),
            pltpu.VMEM(inverses.shape, bf16),
            pltpu.VMEM((strips, cols, cols), bf16),
            pltpu.VMEM((strips, cols, cols), bf16),
            pltpu.VMEM(positions.shape, f32),
            pltpu.VMEM((ITERS, 2, 3, rows, LANES), f32),
            pltpu.VMEM((3, rows, LANES), f32),
            pltpu.VMEM((messages, SUB, cols), f32),
            pltpu.VMEM((messages, SUB, cols), f32),
            pltpu.VMEM((2, rows, cols + 2 * LANES), f32),
            pltpu.VMEM((2, rows, cols + 2 * LANES), f32),
            pltpu.VMEM((cols, cols), f32),
            pltpu.VMEM((cols, cols), f32),
            pltpu.VMEM((cols, cols), bf16),
            pltpu.VMEM((cols, cols), bf16),
            pltpu.VMEM((cols, cols), bf16),
            pltpu.VMEM((cols, cols), bf16),
            pltpu.VMEM((SUB, cols), f32),
            dma((5,)),
            dma((strips,)),
            dma((ITERS, 2)),
            dma((ITERS, 2)),
            dma,
            dma,
            dma((messages,)),
            dma((messages,)),
            dma,
            dma,
        ],
        compiler_params=pltpu.CompilerParams(
            collective_id=0, has_side_effects=True, vmem_limit_bytes=32 * 1024 * 1024),
    )(pin_columns, positions, target, inertia, stiffness, inverses)


def solution(mesh):
    in_specs = (
        P(None, "strip", "col"),
        P(None, "strip", "col"),
        P("strip", "col"),
        P(None, "strip", "col"),
        P(),
        P("strip", None, None),
    )
    out_specs = P(None, "strip", "col")
    run = functools.partial(shards, mesh.shape["strip"], mesh.shape["col"])
    return jax.shard_map(run, mesh=mesh, in_specs=in_specs, out_specs=out_specs, check_vma=False)
```

```python
import functools

import jax
import jax.numpy as jnp
from jax import lax
from jax.experimental import pallas as pl
from jax.experimental.pallas import tpu as pltpu
from jax.sharding import PartitionSpec as P

ITERS = 2

pin_stiffness = 20.0
SUB = 8
LANES = 128
MESH = pl.DeviceIdType.MESH
f32 = jnp.float32
bf16 = jnp.bfloat16


def split(v):
    high = v.astype(bf16).astype(f32)
    return jnp.concatenate([high, v - high], axis=0).astype(bf16)


def folded(product):
    half = product.shape[0] // 2
    return product[:half] + product[half:]


def times_transposed(parts, matrix):
    product = lax.dot_general(
        parts, matrix, (((1,), (1,)), ((), ())), preferred_element_type=f32
    )
    return folded(product)


def times_pair(parts, high, low):
    product = jnp.dot(parts, high, preferred_element_type=f32) + jnp.dot(
        parts, low, preferred_element_type=f32
    )
    return folded(product)


def stretch(squared, rest_len):
    return rest_len * jnp.minimum(lax.rsqrt(squared), 2.0 / rest_len)


def kernel(
    n_strip, n_col,
    pins_in, pos_in, tgt_in, inertia_in, stf_in, inv,
    out,
    pins, pos, tgt, inertia, stf,
    mats, high, low, disp, halo, halo_w, send_row, recv_row, edge_w, cross_w,
    map_send, map_recv, map_high, map_low, both_high, both_low, above_row,
    in_sem, inv_sem, side_send, side_recv, w_send, w_recv, row_send, row_recv, m_send, m_recv,
):
    rows, cols = pos.shape[1], pos.shape[2]
    strips = inv.shape[0]
    srows = rows // strips
    block = srows * cols
    last_start = block - cols
    me_s, me_c = lax.axis_index("strip"), lax.axis_index("col")
    not_top, not_bottom = me_s > 0, me_s < n_strip - 1
    not_left, not_right = me_c > 0, me_c < n_col - 1

    is_tail, is_lead = me_s % 2 == 1, me_s % 2 == 0
    tail_after = is_tail & (me_s + 2 < n_strip)
    tail_before = is_tail & (me_s >= 2)
    lead_before = is_lead & not_top
    mapped_lead = lead_before & not_bottom

    fetches = [
        pltpu.make_async_copy(source, target, in_sem.at[number])
        for number, (source, target) in enumerate((
            (pos_in, pos), (stf_in, stf), (pins_in, pins), (tgt_in, tgt), (inertia_in, inertia)))
    ]
    for fetch in fetches:
        fetch.start()
    loads = [pltpu.make_async_copy(inv.at[k], mats.at[k], inv_sem.at[k]) for k in range(strips)]
    for load in loads:
        load.start()

    barrier = pltpu.get_barrier_semaphore()
    sides = (
        (not_top, (me_s - 1, me_c)),
        (not_bottom, (me_s + 1, me_c)),
        (not_left, (me_s, me_c - 1)),
        (not_right, (me_s, me_c + 1)),
        (tail_before, (me_s - 2, me_c)),
        (tail_after, (me_s + 2, me_c)),
    )
    for there, device in sides:
        @pl.when(there)
        def _():
            pl.semaphore_signal(barrier, inc=1, device_id=device, device_id_type=MESH)

    def side_copies(sweep):
        source = pos if sweep == 0 else disp
        right = pltpu.make_async_remote_copy(
            src_ref=source.at[:, :, pl.ds(cols - LANES, LANES)], dst_ref=halo.at[sweep, 0],
            send_sem=side_send.at[sweep, 0], recv_sem=side_recv.at[sweep, 0],
            device_id=(me_s, me_c + 1), device_id_type=MESH)
        left = pltpu.make_async_remote_copy(
            src_ref=source.at[:, :, pl.ds(0, LANES)], dst_ref=halo.at[sweep, 1],
            send_sem=side_send.at[sweep, 1], recv_sem=side_recv.at[sweep, 1],
            device_id=(me_s, me_c - 1), device_id_type=MESH)
        return right, left

    weights_right = pltpu.make_async_remote_copy(
        src_ref=stf.at[:, :, pl.ds(cols - LANES, LANES)], dst_ref=halo_w,
        send_sem=w_send, recv_sem=w_recv,
        device_id=(me_s, me_c + 1), device_id_type=MESH)

    def row_copy(number, step):
        return pltpu.make_async_remote_copy(
            src_ref=send_row.at[number], dst_ref=recv_row.at[number],
            send_sem=row_send.at[number], recv_sem=row_recv.at[number],
            device_id=(me_s + step, me_c), device_id_type=MESH)

    ups = [row_copy(t, -1) for t in range(ITERS)]
    first_down = row_copy(ITERS, 1)
    base_row = ITERS + 1
    lead_out = [row_copy(base_row + t, 1) for t in range(ITERS)]
    tail_out = [row_copy(base_row + ITERS + t, 2) for t in range(ITERS)]
    next_out = [row_copy(base_row + 2 * ITERS + t, 1) for t in range(ITERS)]
    map_copy = pltpu.make_async_remote_copy(
        src_ref=map_send, dst_ref=map_recv, send_sem=m_send, recv_sem=m_recv,
        device_id=(me_s + 1, me_c), device_id_type=MESH)
    side = [side_copies(t) for t in range(ITERS)]

    row_of = lax.broadcasted_iota(jnp.int32, (SUB, cols), 0)
    field_row = lax.broadcasted_iota(jnp.int32, (rows, cols), 0)

    def compact(parts):
        total = jnp.zeros((SUB, cols), f32)
        for place, part in enumerate(parts):
            total = jnp.where(row_of == place, jnp.broadcast_to(part, (SUB, cols)), total)
        return total

    fetches[0].wait()
    fetches[1].wait()
    send_row[0] = compact([pos[c, 0:1] for c in range(3)])
    send_row[ITERS] = compact(
        [pos[c, rows - 1:rows] for c in range(3)] + [stf[1, rows - 1:rows]])

    @pl.when(jnp.logical_not(not_top))
    def _():
        recv_row[ITERS] = jnp.zeros((SUB, cols), f32)

    @pl.when(jnp.logical_not(not_bottom))
    def _():
        for t in range(ITERS):
            recv_row[t] = jnp.zeros((SUB, cols), f32)

    @pl.when(jnp.logical_not(not_left))
    def _():
        halo_w[...] = jnp.zeros_like(halo_w)
        for t in range(ITERS):
            halo[t, 0] = jnp.zeros((3, rows, LANES), f32)

    @pl.when(jnp.logical_not(not_right))
    def _():
        for t in range(ITERS):
            halo[t, 1] = jnp.zeros((3, rows, LANES), f32)

    w_strip = [stf[1, srows * (k + 1) - 1:srows * (k + 1)] for k in range(strips)]

    def extend_product(first, after):
        for k in range(first, after):
            loads[k].wait()
            matrix = mats[k, last_start:, :cols]
            if k == 0:
                eye = (
                    lax.broadcasted_iota(jnp.int32, (cols, cols), 0)
                    == lax.broadcasted_iota(jnp.int32, (cols, cols), 1)
                ).astype(f32).astype(bf16)
                product = lax.dot_general(
                    eye, matrix, (((1,), (1,)), ((), ())), preferred_element_type=f32)
            else:
                product = times_transposed(
                    jnp.concatenate([high[k - 1], low[k - 1]], axis=0), matrix)
            if k < strips - 1:
                product = product * w_strip[k]
            else:
                map_send[...] = product

                @pl.when(mapped_lead)
                def _():
                    map_copy.start()
            upper = product.astype(bf16)
            high[k] = upper
            low[k] = (product - upper.astype(f32)).astype(bf16)

    extend_product(0, strips // 2)

    neighbours = sum(there.astype(jnp.int32) for there, _ in sides)
    pl.semaphore_wait(barrier, neighbours)

    @pl.when(not_right)
    def _():
        side[0][0].start()
        weights_right.start()

    @pl.when(not_left)
    def _():
        side[0][1].start()

    @pl.when(not_bottom)
    def _():
        first_down.start()

    @pl.when(not_top)
    def _():
        ups[0].start()

    extend_product(strips // 2, strips)

    for fetch in fetches[2:]:
        fetch.wait()
    own_cols = lax.broadcasted_iota(jnp.int32, (1, cols), 1) + me_c * cols
    pinned = jnp.zeros((1, cols), jnp.int32)
    for number in range(pins.shape[0]):
        pinned = pinned | (own_cols == pins[number]).astype(jnp.int32)
    pinned = jnp.broadcast_to(pinned, (rows, cols)) * (field_row == 0) * jnp.where(not_top, 0, 1)
    inertial = [
        inertia[...] * tgt[c] + jnp.where(pinned > 0, pin_stiffness * pos[c], 0.0)
        for c in range(3)
    ]

    wide = cols + 2 * LANES
    wide_lane = lax.broadcasted_iota(jnp.int32, (rows, wide), 1) - LANES
    wide_cols = wide_lane + me_c * cols
    grid_cols = n_col * cols
    vertical = jnp.where(field_row < rows - 1, stf[1], 0.0)
    is_last = field_row % srows == srows - 1
    w_down = jnp.where(is_last, vertical, 0.0)
    w_bottom = jnp.where(not_bottom, stf[1, rows - 1:rows], 0.0)
    rest_row = jnp.where(row_of == 1, 1.0, 0.0)

    def early_rhs(u, left, right, above, w_above):
        field = [jnp.concatenate([left[c], u[c], right[c]], axis=1) for c in range(3)]
        total = [jnp.zeros((rows, wide), f32)] * 3
        for number, offset in enumerate((1, 2)):
            ahead = [pltpu.roll(field[c], wide - offset, axis=1) for c in range(3)]
            gap = [ahead[c] - field[c] for c in range(3)]
            gap[0] = gap[0] + float(offset)
            scale = stretch(gap[0] * gap[0] + gap[1] * gap[1] + gap[2] * gap[2], float(offset))
            weight, cross = edge_w[number], cross_w[number]
            for c in range(3):
                moved = scale * gap[c]
                if c == 0:
                    moved = moved - float(offset)
                pull = weight * moved
                at_a = cross * ahead[c] - pull
                at_b = cross * field[c] + pull
                total[c] = total[c] + at_a + pltpu.roll(at_b, offset, axis=1)
        below = [pltpu.roll(u[c], rows - 1, axis=0) for c in range(3)]
        before = [
            jnp.where(field_row == 0, jnp.broadcast_to(above[c:c + 1], (rows, cols)),
                      pltpu.roll(u[c], 1, axis=0))
            for c in range(3)
        ]
        w_before = jnp.where(
            field_row == 0, jnp.broadcast_to(w_above, (rows, cols)),
            pltpu.roll(stf[1], 1, axis=0))
        gap = [below[c] - u[c] for c in range(3)]
        gap[1] = gap[1] + 1.0
        scale = stretch(gap[0] * gap[0] + gap[1] * gap[1] + gap[2] * gap[2], 1.0)
        back = [u[c] - before[c] for c in range(3)]
        back[1] = back[1] + 1.0
        back_scale = stretch(back[0] * back[0] + back[1] * back[1] + back[2] * back[2], 1.0)
        result = []
        for c in range(3):
            rest = 1.0 if c == 1 else 0.0
            value = inertial[c] + total[c][:, LANES:LANES + cols]
            value = value - vertical * (scale * gap[c] - rest) + w_down * below[c]
            result.append(value + w_before * (back_scale * back[c] - rest))
        return result

    def late_rhs(last_rows, below):
        gap = below - last_rows + rest_row
        scale = stretch(jnp.sum(gap * gap, axis=0, keepdims=True), 1.0)
        return w_bottom * (below - scale * gap + rest_row)

    def strip_vector(rhs, k):
        return [
            compact([rhs[c][srows * k + i:srows * k + i + 1] for c in range(3)])
            for i in range(srows)
        ]

    def receive(copy, there):
        @pl.when(there)
        def _():
            copy.wait_recv()

    def send(copy, there):
        @pl.when(there)
        def _():
            copy.start()

    @pl.when(not_left)
    def _():
        weights_right.wait_recv()

    for number, (offset, channel) in enumerate(((1, 0), (2, 2))):
        weight = jnp.concatenate(
            [halo_w[channel], stf[channel], jnp.zeros((rows, LANES), f32)], axis=1)
        inside = (wide_cols >= 0) & (wide_cols + offset <= grid_cols - 1)
        weight = jnp.where(inside, weight, 0.0)
        crossing = ((wide_lane < 0) & (wide_lane + offset >= 0)) | (
            (wide_lane < cols) & (wide_lane + offset >= cols))
        edge_w[number] = weight
        cross_w[number] = jnp.where(crossing, weight, 0.0)

    receive(first_down, not_top)
    above = recv_row[ITERS]
    w_above = jnp.where(not_top, above[3:4], 0.0)
    current = [pos[c] for c in range(3)]
    last_rows = compact([pos[c, rows - 1:rows] for c in range(3)])

    for sweep in range(ITERS):
        receive(side[sweep][0], not_left)
        receive(side[sweep][1], not_right)
        rhs = early_rhs(
            current, [halo[sweep, 0, c] for c in range(3)], [halo[sweep, 1, c] for c in range(3)],
            above, w_above)
        vectors = [strip_vector(rhs, k) for k in range(strips)]
        if sweep == 0:
            receive(ups[sweep], not_bottom)
            vectors[-1][-1] = vectors[-1][-1] + late_rhs(last_rows, recv_row[sweep])
        base, offsets = [], []
        for k in range(strips):
            parts = split(jnp.concatenate(vectors[k], axis=1))
            base.append(times_transposed(parts, mats[k]))
        carried = None
        for k in range(strips):
            if k == 0:
                carried = base[k][:, last_start:]
            else:
                carried = base[k][:, last_start:] + times_transposed(
                    split(carried), mats[k, last_start:, :cols])
            if k < strips - 1:
                carried = carried * w_strip[k]
            offsets.append(carried)
        if sweep > 0:
            receive(ups[sweep], not_bottom)
            late = split(late_rhs(last_rows, recv_row[sweep]))
            change = times_transposed(late, mats[strips - 1, :, last_start:])
            base[-1] = base[-1] + change
            offsets[-1] = offsets[-1] + change[:, last_start:]

        send_row[base_row + sweep] = offsets[-1]
        send(lead_out[sweep], is_lead & not_bottom)

        def pass_on(tail_rows):
            send_row[base_row + ITERS + sweep] = tail_rows * w_bottom
            send_row[base_row + 2 * ITERS + sweep] = tail_rows
            send(tail_out[sweep], tail_after)
            send(next_out[sweep], is_tail & not_bottom)

        @pl.when(is_tail)
        def _():
            lead_out[sweep].wait_recv()
            lead_rows = recv_row[base_row + sweep]
            tail_rows = offsets[-1] + times_pair(
                split(lead_rows * w_above), high[strips - 1], low[strips - 1])

            @pl.when(jnp.logical_not(tail_before))
            def _():
                pass_on(tail_rows)
                above_row[...] = lead_rows

            @pl.when(tail_before)
            def _():
                if sweep == 0:
                    map_copy.wait_recv()
                    received = map_recv[...]
                    upper = received.astype(bf16)
                    map_high[...] = upper
                    map_low[...] = (received - upper.astype(f32)).astype(bf16)
                    both = times_pair(
                        split(received * w_above), high[strips - 1], low[strips - 1])
                    upper = both.astype(bf16)
                    both_high[...] = upper
                    both_low[...] = (both - upper.astype(f32)).astype(bf16)
                tail_out[sweep].wait_recv()
                entering = split(recv_row[base_row + ITERS + sweep])
                pass_on(tail_rows + times_pair(entering, both_high[...], both_low[...]))
                above_row[...] = lead_rows + times_pair(entering, map_high[...], map_low[...])

        @pl.when(lead_before)
        def _():
            next_out[sweep].wait_recv()
            above_row[...] = recv_row[base_row + 2 * ITERS + sweep]

        @pl.when(jnp.logical_not(not_top))
        def _():
            above_row[...] = jnp.zeros((SUB, cols), f32)

        above = above_row[...]
        entering = split(above * w_above)
        solved = [base[0] + times_transposed(entering, mats[0, :, :cols])]
        if sweep < ITERS - 1:
            send_row[sweep + 1] = solved[0][:, :cols]
            send(ups[sweep + 1], not_top)
        for k in range(1, strips):
            carried = offsets[k - 1] + times_pair(entering, high[k - 1], low[k - 1])
            solved.append(base[k] + times_transposed(split(carried), mats[k, :, :cols]))
        last_rows = solved[-1][:, last_start:]
        current = []
        for c in range(3):
            field = jnp.zeros((rows, cols), f32)
            for k in range(strips):
                for i in range(srows):
                    row = solved[k][c:c + 1, i * cols:(i + 1) * cols]
                    field = jnp.where(
                        field_row == srows * k + i, jnp.broadcast_to(row, (rows, cols)), field)
            current.append(field)
            if sweep < ITERS - 1:
                disp[c] = field
            else:
                out[c] = field
        if sweep < ITERS - 1:
            send(side[sweep + 1][0], not_right)
            send(side[sweep + 1][1], not_left)

    def sent(copy, there):
        @pl.when(there)
        def _():
            copy.wait_send()

    sent(weights_right, not_right)
    for right, left in side:
        sent(right, not_right)
        sent(left, not_left)
    for copy in ups:
        sent(copy, not_top)
    sent(first_down, not_bottom)
    sent(map_copy, mapped_lead)
    for t in range(ITERS):
        sent(lead_out[t], is_lead & not_bottom)
        sent(tail_out[t], tail_after)
        sent(next_out[t], is_tail & not_bottom)


def shards(n_strip, n_col, positions, target, inertia, stiffness, pin_columns, inverses):
    rows, cols = positions.shape[1:]
    strips, block, _ = inverses.shape
    messages = 4 * ITERS + 1
    dma = pltpu.SemaphoreType.DMA
    return pl.pallas_call(
        functools.partial(kernel, n_strip, n_col),
        out_shape=jax.ShapeDtypeStruct(positions.shape, f32),
        in_specs=[pl.BlockSpec(memory_space=pltpu.HBM)] * 6,
        out_specs=pl.BlockSpec(memory_space=pltpu.VMEM),
        scratch_shapes=[
            pltpu.SMEM(pin_columns.shape, jnp.int32),
            pltpu.VMEM(positions.shape, f32),
            pltpu.VMEM(target.shape, f32),
            pltpu.VMEM(inertia.shape, f32),
            pltpu.VMEM(stiffness.shape, f32),
            pltpu.VMEM(inverses.shape, bf16),
            pltpu.VMEM((strips, cols, cols), bf16),
            pltpu.VMEM((strips, cols, cols), bf16),
            pltpu.VMEM(positions.shape, f32),
            pltpu.VMEM((ITERS, 2, 3, rows, LANES), f32),
            pltpu.VMEM((3, rows, LANES), f32),
            pltpu.VMEM((messages, SUB, cols), f32),
            pltpu.VMEM((messages, SUB, cols), f32),
            pltpu.VMEM((2, rows, cols + 2 * LANES), f32),
            pltpu.VMEM((2, rows, cols + 2 * LANES), f32),
            pltpu.VMEM((cols, cols), f32),
            pltpu.VMEM((cols, cols), f32),
            pltpu.VMEM((cols, cols), bf16),
            pltpu.VMEM((cols, cols), bf16),
            pltpu.VMEM((cols, cols), bf16),
            pltpu.VMEM((cols, cols), bf16),
            pltpu.VMEM((SUB, cols), f32),
            dma((5,)),
            dma((strips,)),
            dma((ITERS, 2)),
            dma((ITERS, 2)),
            dma,
            dma,
            dma((messages,)),
            dma((messages,)),
            dma,
            dma,
        ],
        compiler_params=pltpu.CompilerParams(
            collective_id=0, has_side_effects=True, vmem_limit_bytes=67_000_000),
    )(pin_columns, positions, target, inertia, stiffness, inverses)


def solution(mesh):
    in_specs = (
        P(None, "strip", "col"),
        P(None, "strip", "col"),
        P("strip", "col"),
        P(None, "strip", "col"),
        P(),
        P("strip", None, None),
    )
    out_specs = P(None, "strip", "col")
    run = functools.partial(shards, mesh.shape["strip"], mesh.shape["col"])
    return jax.shard_map(run, mesh=mesh, in_specs=in_specs, out_specs=out_specs, check_vma=False)
```

```python
import functools

import jax
import jax.numpy as jnp
from jax import lax
from jax.experimental import pallas as pl
from jax.experimental.pallas import tpu as pltpu
from jax.sharding import PartitionSpec as P

ITERS = 2

pin_stiffness = 20.0
SUB = 8
LANES = 128
MESH = pl.DeviceIdType.MESH
f32 = jnp.float32
bf16 = jnp.bfloat16


def split(v):
    high = v.astype(bf16).astype(f32)
    return jnp.concatenate([high, v - high], axis=0).astype(bf16)


def folded(product):
    half = product.shape[0] // 2
    return product[:half] + product[half:]


def times_transposed(parts, matrix):
    product = lax.dot_general(
        parts, matrix, (((1,), (1,)), ((), ())), preferred_element_type=f32
    )
    return folded(product)


def times_pair(parts, high, low):
    product = jnp.dot(parts, high, preferred_element_type=f32) + jnp.dot(
        parts, low, preferred_element_type=f32
    )
    return folded(product)


def stretch(squared, rest_len):
    return rest_len * jnp.minimum(lax.rsqrt(squared), 2.0 / rest_len)


def kernel(
    n_strip, n_col,
    pins_in, pos_in, tgt_in, inertia_in, stf_in, inv,
    out,
    pins, pos, tgt, inertia, stf,
    mats, high, low, disp, halo, halo_w, send_row, recv_row, edge_w, cross_w,
    map_send, map_recv, map_high, map_low, both_high, both_low, above_row, late_change,
    in_sem, inv_sem, side_send, side_recv, w_send, w_recv, row_send, row_recv, m_send, m_recv,
):
    rows, cols = pos.shape[1], pos.shape[2]
    strips = inv.shape[0]
    srows = rows // strips
    block = srows * cols
    last_start = block - cols
    me_s, me_c = lax.axis_index("strip"), lax.axis_index("col")
    not_top, not_bottom = me_s > 0, me_s < n_strip - 1
    not_left, not_right = me_c > 0, me_c < n_col - 1

    is_tail, is_lead = me_s % 2 == 1, me_s % 2 == 0
    tail_after = is_tail & (me_s + 2 < n_strip)
    tail_before = is_tail & (me_s >= 2)
    lead_before = is_lead & not_top
    mapped_lead = lead_before & not_bottom

    fetches = [
        pltpu.make_async_copy(source, target, in_sem.at[number])
        for number, (source, target) in enumerate((
            (pos_in, pos), (stf_in, stf), (pins_in, pins), (tgt_in, tgt), (inertia_in, inertia)))
    ]
    for fetch in fetches:
        fetch.start()
    loads = [pltpu.make_async_copy(inv.at[k], mats.at[k], inv_sem.at[k]) for k in range(strips)]
    for load in loads:
        load.start()

    barrier = pltpu.get_barrier_semaphore()
    sides = (
        (not_top, (me_s - 1, me_c)),
        (not_bottom, (me_s + 1, me_c)),
        (not_left, (me_s, me_c - 1)),
        (not_right, (me_s, me_c + 1)),
        (tail_before, (me_s - 2, me_c)),
        (tail_after, (me_s + 2, me_c)),
    )
    for there, device in sides:
        @pl.when(there)
        def _():
            pl.semaphore_signal(barrier, inc=1, device_id=device, device_id_type=MESH)

    def side_copies(sweep):
        source = pos if sweep == 0 else disp
        right = pltpu.make_async_remote_copy(
            src_ref=source.at[:, :, pl.ds(cols - LANES, LANES)], dst_ref=halo.at[sweep, 0],
            send_sem=side_send.at[sweep, 0], recv_sem=side_recv.at[sweep, 0],
            device_id=(me_s, me_c + 1), device_id_type=MESH)
        left = pltpu.make_async_remote_copy(
            src_ref=source.at[:, :, pl.ds(0, LANES)], dst_ref=halo.at[sweep, 1],
            send_sem=side_send.at[sweep, 1], recv_sem=side_recv.at[sweep, 1],
            device_id=(me_s, me_c - 1), device_id_type=MESH)
        return right, left

    weights_right = pltpu.make_async_remote_copy(
        src_ref=stf.at[:, :, pl.ds(cols - LANES, LANES)], dst_ref=halo_w,
        send_sem=w_send, recv_sem=w_recv,
        device_id=(me_s, me_c + 1), device_id_type=MESH)

    def row_copy(number, step):
        return pltpu.make_async_remote_copy(
            src_ref=send_row.at[number], dst_ref=recv_row.at[number],
            send_sem=row_send.at[number], recv_sem=row_recv.at[number],
            device_id=(me_s + step, me_c), device_id_type=MESH)

    ups = [row_copy(t, -1) for t in range(ITERS)]
    first_down = row_copy(ITERS, 1)
    base_row = ITERS + 1
    lead_out = [row_copy(base_row + t, 1) for t in range(ITERS)]
    tail_out = [row_copy(base_row + ITERS + t, 2) for t in range(ITERS)]
    next_out = [row_copy(base_row + 2 * ITERS + t, 1) for t in range(ITERS)]
    map_copy = pltpu.make_async_remote_copy(
        src_ref=map_send, dst_ref=map_recv, send_sem=m_send, recv_sem=m_recv,
        device_id=(me_s + 1, me_c), device_id_type=MESH)
    side = [side_copies(t) for t in range(ITERS)]

    row_of = lax.broadcasted_iota(jnp.int32, (SUB, cols), 0)
    field_row = lax.broadcasted_iota(jnp.int32, (rows, cols), 0)

    def compact(parts):
        total = jnp.zeros((SUB, cols), f32)
        for place, part in enumerate(parts):
            total = jnp.where(row_of == place, jnp.broadcast_to(part, (SUB, cols)), total)
        return total

    fetches[0].wait()
    fetches[1].wait()
    send_row[0] = compact([pos[c, 0:1] for c in range(3)])
    send_row[ITERS] = compact(
        [pos[c, rows - 1:rows] for c in range(3)] + [stf[1, rows - 1:rows]])

    @pl.when(jnp.logical_not(not_top))
    def _():
        recv_row[ITERS] = jnp.zeros((SUB, cols), f32)

    @pl.when(jnp.logical_not(not_bottom))
    def _():
        late_change[...] = jnp.zeros_like(late_change)
        for t in range(ITERS):
            recv_row[t] = jnp.zeros((SUB, cols), f32)

    @pl.when(jnp.logical_not(not_left))
    def _():
        halo_w[...] = jnp.zeros_like(halo_w)
        for t in range(ITERS):
            halo[t, 0] = jnp.zeros((3, rows, LANES), f32)

    @pl.when(jnp.logical_not(not_right))
    def _():
        for t in range(ITERS):
            halo[t, 1] = jnp.zeros((3, rows, LANES), f32)

    w_strip = [stf[1, srows * (k + 1) - 1:srows * (k + 1)] for k in range(strips)]

    def extend_product(first, after):
        for k in range(first, after):
            loads[k].wait()
            matrix = mats[k, last_start:, :cols]
            if k == 0:
                eye = (
                    lax.broadcasted_iota(jnp.int32, (cols, cols), 0)
                    == lax.broadcasted_iota(jnp.int32, (cols, cols), 1)
                ).astype(f32).astype(bf16)
                product = lax.dot_general(
                    eye, matrix, (((1,), (1,)), ((), ())), preferred_element_type=f32)
            else:
                product = times_transposed(
                    jnp.concatenate([high[k - 1], low[k - 1]], axis=0), matrix)
            if k < strips - 1:
                product = product * w_strip[k]
            else:
                map_send[...] = product

                @pl.when(mapped_lead)
                def _():
                    map_copy.start()
            upper = product.astype(bf16)
            high[k] = upper
            low[k] = (product - upper.astype(f32)).astype(bf16)

    extend_product(0, strips // 2)

    neighbours = sum(there.astype(jnp.int32) for there, _ in sides)
    pl.semaphore_wait(barrier, neighbours)

    @pl.when(not_right)
    def _():
        side[0][0].start()
        weights_right.start()

    @pl.when(not_left)
    def _():
        side[0][1].start()

    @pl.when(not_bottom)
    def _():
        first_down.start()

    @pl.when(not_top)
    def _():
        ups[0].start()

    extend_product(strips // 2, strips)

    for fetch in fetches[2:]:
        fetch.wait()
    own_cols = lax.broadcasted_iota(jnp.int32, (1, cols), 1) + me_c * cols
    pinned = jnp.zeros((1, cols), jnp.int32)
    for number in range(pins.shape[0]):
        pinned = pinned | (own_cols == pins[number]).astype(jnp.int32)
    pinned = jnp.broadcast_to(pinned, (rows, cols)) * (field_row == 0) * jnp.where(not_top, 0, 1)
    inertial = [
        inertia[...] * tgt[c] + jnp.where(pinned > 0, pin_stiffness * pos[c], 0.0)
        for c in range(3)
    ]

    wide = cols + 2 * LANES
    wide_lane = lax.broadcasted_iota(jnp.int32, (rows, wide), 1) - LANES
    wide_cols = wide_lane + me_c * cols
    grid_cols = n_col * cols
    vertical = jnp.where(field_row < rows - 1, stf[1], 0.0)
    is_last = field_row % srows == srows - 1
    w_down = jnp.where(is_last, vertical, 0.0)
    w_bottom = jnp.where(not_bottom, stf[1, rows - 1:rows], 0.0)
    rest_row = jnp.where(row_of == 1, 1.0, 0.0)

    def early_rhs(u, left, right, above, w_above):
        field = [jnp.concatenate([left[c], u[c], right[c]], axis=1) for c in range(3)]
        total = [jnp.zeros((rows, wide), f32)] * 3
        for number, offset in enumerate((1, 2)):
            ahead = [pltpu.roll(field[c], wide - offset, axis=1) for c in range(3)]
            gap = [ahead[c] - field[c] for c in range(3)]
            gap[0] = gap[0] + float(offset)
            scale = stretch(gap[0] * gap[0] + gap[1] * gap[1] + gap[2] * gap[2], float(offset))
            weight, cross = edge_w[number], cross_w[number]
            for c in range(3):
                moved = scale * gap[c]
                if c == 0:
                    moved = moved - float(offset)
                pull = weight * moved
                at_a = cross * ahead[c] - pull
                at_b = cross * field[c] + pull
                total[c] = total[c] + at_a + pltpu.roll(at_b, offset, axis=1)
        below = [pltpu.roll(u[c], rows - 1, axis=0) for c in range(3)]
        before = [
            jnp.where(field_row == 0, jnp.broadcast_to(above[c:c + 1], (rows, cols)),
                      pltpu.roll(u[c], 1, axis=0))
            for c in range(3)
        ]
        w_before = jnp.where(
            field_row == 0, jnp.broadcast_to(w_above, (rows, cols)),
            pltpu.roll(stf[1], 1, axis=0))
        gap = [below[c] - u[c] for c in range(3)]
        gap[1] = gap[1] + 1.0
        scale = stretch(gap[0] * gap[0] + gap[1] * gap[1] + gap[2] * gap[2], 1.0)
        back = [u[c] - before[c] for c in range(3)]
        back[1] = back[1] + 1.0
        back_scale = stretch(back[0] * back[0] + back[1] * back[1] + back[2] * back[2], 1.0)
        result = []
        for c in range(3):
            rest = 1.0 if c == 1 else 0.0
            value = inertial[c] + total[c][:, LANES:LANES + cols]
            value = value - vertical * (scale * gap[c] - rest) + w_down * below[c]
            result.append(value + w_before * (back_scale * back[c] - rest))
        return result

    def late_rhs(last_rows, below):
        gap = below - last_rows + rest_row
        scale = stretch(jnp.sum(gap * gap, axis=0, keepdims=True), 1.0)
        return w_bottom * (below - scale * gap + rest_row)

    def strip_vector(rhs, k):
        return [
            compact([rhs[c][srows * k + i:srows * k + i + 1] for c in range(3)])
            for i in range(srows)
        ]

    def receive(copy, there):
        @pl.when(there)
        def _():
            copy.wait_recv()

    def send(copy, there):
        @pl.when(there)
        def _():
            copy.start()

    @pl.when(not_left)
    def _():
        weights_right.wait_recv()

    for number, (offset, channel) in enumerate(((1, 0), (2, 2))):
        weight = jnp.concatenate(
            [halo_w[channel], stf[channel], jnp.zeros((rows, LANES), f32)], axis=1)
        inside = (wide_cols >= 0) & (wide_cols + offset <= grid_cols - 1)
        weight = jnp.where(inside, weight, 0.0)
        crossing = ((wide_lane < 0) & (wide_lane + offset >= 0)) | (
            (wide_lane < cols) & (wide_lane + offset >= cols))
        edge_w[number] = weight
        cross_w[number] = jnp.where(crossing, weight, 0.0)

    receive(first_down, not_top)
    above = recv_row[ITERS]
    w_above = jnp.where(not_top, above[3:4], 0.0)
    current = [pos[c] for c in range(3)]
    last_rows = compact([pos[c, rows - 1:rows] for c in range(3)])

    for sweep in range(ITERS):
        receive(side[sweep][0], not_left)
        receive(side[sweep][1], not_right)
        rhs = early_rhs(
            current, [halo[sweep, 0, c] for c in range(3)], [halo[sweep, 1, c] for c in range(3)],
            above, w_above)
        vectors = [strip_vector(rhs, k) for k in range(strips)]
        if sweep == 0:
            receive(ups[sweep], not_bottom)
            vectors[-1][-1] = vectors[-1][-1] + late_rhs(last_rows, recv_row[sweep])
        base, offsets = [], []
        for k in range(strips):
            parts = split(jnp.concatenate(vectors[k], axis=1))
            base.append(times_transposed(parts, mats[k]))
        carried = None
        for k in range(strips):
            if k == 0:
                carried = base[k][:, last_start:]
            else:
                carried = base[k][:, last_start:] + times_transposed(
                    split(carried), mats[k, last_start:, :cols])
            if k < strips - 1:
                carried = carried * w_strip[k]
            offsets.append(carried)
        def add_late():
            if sweep == 0:
                return 0.0
            ups[sweep].wait_recv()
            late = split(late_rhs(last_rows, recv_row[sweep]))
            change = times_transposed(late, mats[strips - 1, :, last_start:])
            late_change[...] = change
            return change[:, last_start:]

        @pl.when(is_lead & not_bottom)
        def _():
            send_row[base_row + sweep] = offsets[-1] + add_late()
            lead_out[sweep].start()

        def pass_on(tail_rows):
            send_row[base_row + ITERS + sweep] = tail_rows * w_bottom
            send_row[base_row + 2 * ITERS + sweep] = tail_rows
            send(tail_out[sweep], tail_after)
            send(next_out[sweep], is_tail & not_bottom)

        @pl.when(is_tail)
        def _():
            lead_out[sweep].wait_recv()
            lead_rows = recv_row[base_row + sweep]
            tail_rows = offsets[-1] + times_pair(
                split(lead_rows * w_above), high[strips - 1], low[strips - 1])

            @pl.when(jnp.logical_not(tail_before))
            def _():
                @pl.when(not_bottom)
                def _():
                    pass_on(tail_rows + add_late())

                above_row[...] = lead_rows

            @pl.when(tail_before)
            def _():
                if sweep == 0:
                    map_copy.wait_recv()
                    received = map_recv[...]
                    upper = received.astype(bf16)
                    map_high[...] = upper
                    map_low[...] = (received - upper.astype(f32)).astype(bf16)
                    both = times_pair(
                        split(received * w_above), high[strips - 1], low[strips - 1])
                    upper = both.astype(bf16)
                    both_high[...] = upper
                    both_low[...] = (both - upper.astype(f32)).astype(bf16)
                tail_out[sweep].wait_recv()
                entering = split(recv_row[base_row + ITERS + sweep])

                @pl.when(not_bottom)
                def _():
                    onward = tail_rows + times_pair(entering, both_high[...], both_low[...])
                    pass_on(onward + add_late())

                above_row[...] = lead_rows + times_pair(entering, map_high[...], map_low[...])

        @pl.when(lead_before)
        def _():
            next_out[sweep].wait_recv()
            above_row[...] = recv_row[base_row + 2 * ITERS + sweep]

        @pl.when(jnp.logical_not(not_top))
        def _():
            above_row[...] = jnp.zeros((SUB, cols), f32)

        if sweep > 0:
            base[-1] = base[-1] + late_change[...]
        above = above_row[...]
        entering = split(above * w_above)
        solved = [base[0] + times_transposed(entering, mats[0, :, :cols])]
        if sweep < ITERS - 1:
            send_row[sweep + 1] = solved[0][:, :cols]
            send(ups[sweep + 1], not_top)
        for k in range(1, strips):
            carried = offsets[k - 1] + times_pair(entering, high[k - 1], low[k - 1])
            solved.append(base[k] + times_transposed(split(carried), mats[k, :, :cols]))
        last_rows = solved[-1][:, last_start:]
        current = []
        for c in range(3):
            field = jnp.zeros((rows, cols), f32)
            for k in range(strips):
                for i in range(srows):
                    row = solved[k][c:c + 1, i * cols:(i + 1) * cols]
                    field = jnp.where(
                        field_row == srows * k + i, jnp.broadcast_to(row, (rows, cols)), field)
            current.append(field)
            if sweep < ITERS - 1:
                disp[c] = field
            else:
                out[c] = field
        if sweep < ITERS - 1:
            send(side[sweep + 1][0], not_right)
            send(side[sweep + 1][1], not_left)

    def sent(copy, there):
        @pl.when(there)
        def _():
            copy.wait_send()

    sent(weights_right, not_right)
    for right, left in side:
        sent(right, not_right)
        sent(left, not_left)
    for copy in ups:
        sent(copy, not_top)
    sent(first_down, not_bottom)
    sent(map_copy, mapped_lead)
    for t in range(ITERS):
        sent(lead_out[t], is_lead & not_bottom)
        sent(tail_out[t], tail_after)
        sent(next_out[t], is_tail & not_bottom)


def shards(n_strip, n_col, positions, target, inertia, stiffness, pin_columns, inverses):
    rows, cols = positions.shape[1:]
    strips, block, _ = inverses.shape
    messages = 4 * ITERS + 1
    dma = pltpu.SemaphoreType.DMA
    return pl.pallas_call(
        functools.partial(kernel, n_strip, n_col),
        out_shape=pltpu.VMEM(positions.shape, f32),
        in_specs=[pl.BlockSpec(memory_space=pltpu.HBM)] * 6,
        out_specs=pl.BlockSpec(memory_space=pltpu.VMEM),
        scratch_shapes=[
            pltpu.SMEM(pin_columns.shape, jnp.int32),
            pltpu.VMEM(positions.shape, f32),
            pltpu.VMEM(target.shape, f32),
            pltpu.VMEM(inertia.shape, f32),
            pltpu.VMEM(stiffness.shape, f32),
            pltpu.VMEM(inverses.shape, bf16),
            pltpu.VMEM((strips, cols, cols), bf16),
            pltpu.VMEM((strips, cols, cols), bf16),
            pltpu.VMEM(positions.shape, f32),
            pltpu.VMEM((ITERS, 2, 3, rows, LANES), f32),
            pltpu.VMEM((3, rows, LANES), f32),
            pltpu.VMEM((messages, SUB, cols), f32),
            pltpu.VMEM((messages, SUB, cols), f32),
            pltpu.VMEM((2, rows, cols + 2 * LANES), f32),
            pltpu.VMEM((2, rows, cols + 2 * LANES), f32),
            pltpu.VMEM((cols, cols), f32),
            pltpu.VMEM((cols, cols), f32),
            pltpu.VMEM((cols, cols), bf16),
            pltpu.VMEM((cols, cols), bf16),
            pltpu.VMEM((cols, cols), bf16),
            pltpu.VMEM((cols, cols), bf16),
            pltpu.VMEM((SUB, cols), f32),
            pltpu.VMEM((SUB, block), f32),
            dma((5,)),
            dma((strips,)),
            dma((ITERS, 2)),
            dma((ITERS, 2)),
            dma,
            dma,
            dma((messages,)),
            dma((messages,)),
            dma,
            dma,
        ],
        compiler_params=pltpu.CompilerParams(
            collective_id=0, has_side_effects=True, vmem_limit_bytes=67_000_000),
    )(pin_columns, positions, target, inertia, stiffness, inverses)


def solution(mesh):
    in_specs = (
        P(None, "strip", "col"),
        P(None, "strip", "col"),
        P("strip", "col"),
        P(None, "strip", "col"),
        P(),
        P("strip", None, None),
    )
    out_specs = P(None, "strip", "col")
    run = functools.partial(shards, mesh.shape["strip"], mesh.shape["col"])
    return jax.shard_map(run, mesh=mesh, in_specs=in_specs, out_specs=out_specs, check_vma=False)
```

```python
import functools

import jax
import jax.numpy as jnp
from jax import lax
from jax.experimental import pallas as pl
from jax.experimental.pallas import tpu as pltpu
from jax.sharding import PartitionSpec as P

ITERS = 2

pin_stiffness = 20.0
SUB = 8
LANES = 128
MESH = pl.DeviceIdType.MESH
f32 = jnp.float32
bf16 = jnp.bfloat16


def split(v):
    high = v.astype(bf16).astype(f32)
    return jnp.concatenate([high, v - high], axis=0).astype(bf16)


def folded(product):
    half = product.shape[0] // 2
    return product[:half] + product[half:]


def times_transposed(parts, matrix):
    product = lax.dot_general(
        parts, matrix, (((1,), (1,)), ((), ())), preferred_element_type=f32
    )
    return folded(product)


def times_pair(parts, high, low):
    product = jnp.dot(parts, high, preferred_element_type=f32) + jnp.dot(
        parts, low, preferred_element_type=f32
    )
    return folded(product)


def stretch(squared, rest_len):
    return rest_len * jnp.minimum(lax.rsqrt(squared), 2.0 / rest_len)


def kernel(
    n_strip, n_col,
    pins_in, pos_in, tgt_in, inertia_in, stf_in, inv,
    out,
    pins, pos, tgt, inertia, stf,
    mats, high, low, disp, halo, halo_w, send_row, recv_row, edge_w, cross_w,
    map_send, map_recv, map_high, map_low, both_high, both_low, above_row, late_change,
    in_sem, inv_sem, side_send, side_recv, w_send, w_recv, row_send, row_recv, m_send, m_recv,
):
    rows, cols = pos.shape[1], pos.shape[2]
    strips = inv.shape[0]
    srows = rows // strips
    block = srows * cols
    last_start = block - cols
    me_s, me_c = lax.axis_index("strip"), lax.axis_index("col")
    not_top, not_bottom = me_s > 0, me_s < n_strip - 1
    not_left, not_right = me_c > 0, me_c < n_col - 1

    is_tail, is_lead = me_s % 2 == 1, me_s % 2 == 0
    tail_after = is_tail & (me_s + 2 < n_strip)
    tail_before = is_tail & (me_s >= 2)
    lead_before = is_lead & not_top
    mapped_lead = lead_before & not_bottom

    fetches = [
        pltpu.make_async_copy(source, target, in_sem.at[number])
        for number, (source, target) in enumerate((
            (pos_in, pos), (stf_in, stf), (pins_in, pins), (tgt_in, tgt), (inertia_in, inertia)))
    ]
    for fetch in fetches:
        fetch.start()
    loads = [pltpu.make_async_copy(inv.at[k], mats.at[k], inv_sem.at[k]) for k in range(strips)]
    for load in loads:
        load.start()

    barrier = pltpu.get_barrier_semaphore()
    sides = (
        (not_top, (me_s - 1, me_c)),
        (not_bottom, (me_s + 1, me_c)),
        (not_left, (me_s, me_c - 1)),
        (not_right, (me_s, me_c + 1)),
        (tail_before, (me_s - 2, me_c)),
        (tail_after, (me_s + 2, me_c)),
    )
    for there, device in sides:
        @pl.when(there)
        def _():
            pl.semaphore_signal(barrier, inc=1, device_id=device, device_id_type=MESH)

    def side_copies(sweep):
        source = pos if sweep == 0 else disp
        right = pltpu.make_async_remote_copy(
            src_ref=source.at[:, :, pl.ds(cols - LANES, LANES)], dst_ref=halo.at[sweep, 0],
            send_sem=side_send.at[sweep, 0], recv_sem=side_recv.at[sweep, 0],
            device_id=(me_s, me_c + 1), device_id_type=MESH)
        left = pltpu.make_async_remote_copy(
            src_ref=source.at[:, :, pl.ds(0, LANES)], dst_ref=halo.at[sweep, 1],
            send_sem=side_send.at[sweep, 1], recv_sem=side_recv.at[sweep, 1],
            device_id=(me_s, me_c - 1), device_id_type=MESH)
        return right, left

    weights_right = pltpu.make_async_remote_copy(
        src_ref=stf.at[:, :, pl.ds(cols - LANES, LANES)], dst_ref=halo_w,
        send_sem=w_send, recv_sem=w_recv,
        device_id=(me_s, me_c + 1), device_id_type=MESH)

    def row_copy(number, step):
        return pltpu.make_async_remote_copy(
            src_ref=send_row.at[number], dst_ref=recv_row.at[number],
            send_sem=row_send.at[number], recv_sem=row_recv.at[number],
            device_id=(me_s + step, me_c), device_id_type=MESH)

    ups = [row_copy(t, -1) for t in range(ITERS)]
    first_down = row_copy(ITERS, 1)
    base_row = ITERS + 1
    lead_out = [row_copy(base_row + t, 1) for t in range(ITERS)]
    tail_out = [row_copy(base_row + ITERS + t, 2) for t in range(ITERS)]
    next_out = [row_copy(base_row + 2 * ITERS + t, 1) for t in range(ITERS)]
    map_copy = pltpu.make_async_remote_copy(
        src_ref=map_send, dst_ref=map_recv, send_sem=m_send, recv_sem=m_recv,
        device_id=(me_s + 1, me_c), device_id_type=MESH)
    side = [side_copies(t) for t in range(ITERS)]

    row_of = lax.broadcasted_iota(jnp.int32, (SUB, cols), 0)
    field_row = lax.broadcasted_iota(jnp.int32, (rows, cols), 0)

    def compact(parts):
        total = jnp.zeros((SUB, cols), f32)
        for place, part in enumerate(parts):
            total = jnp.where(row_of == place, jnp.broadcast_to(part, (SUB, cols)), total)
        return total

    fetches[0].wait()
    fetches[1].wait()
    send_row[0] = compact([pos[c, 0:1] for c in range(3)])
    send_row[ITERS] = compact(
        [pos[c, rows - 1:rows] for c in range(3)] + [stf[1, rows - 1:rows]])

    @pl.when(jnp.logical_not(not_top))
    def _():
        recv_row[ITERS] = jnp.zeros((SUB, cols), f32)

    @pl.when(jnp.logical_not(not_bottom))
    def _():
        late_change[...] = jnp.zeros_like(late_change)
        for t in range(ITERS):
            recv_row[t] = jnp.zeros((SUB, cols), f32)

    @pl.when(jnp.logical_not(not_left))
    def _():
        halo_w[...] = jnp.zeros_like(halo_w)
        for t in range(ITERS):
            halo[t, 0] = jnp.zeros((3, rows, LANES), f32)

    @pl.when(jnp.logical_not(not_right))
    def _():
        for t in range(ITERS):
            halo[t, 1] = jnp.zeros((3, rows, LANES), f32)

    w_strip = [stf[1, srows * (k + 1) - 1:srows * (k + 1)] for k in range(strips)]

    def extend_product(first, after):
        for k in range(first, after):
            loads[k].wait()
            matrix = mats[k, last_start:, :cols]
            if k == 0:
                eye = (
                    lax.broadcasted_iota(jnp.int32, (cols, cols), 0)
                    == lax.broadcasted_iota(jnp.int32, (cols, cols), 1)
                ).astype(f32).astype(bf16)
                product = lax.dot_general(
                    eye, matrix, (((1,), (1,)), ((), ())), preferred_element_type=f32)
            else:
                product = times_transposed(
                    jnp.concatenate([high[k - 1], low[k - 1]], axis=0), matrix)
            if k < strips - 1:
                product = product * w_strip[k]
            else:
                map_send[...] = product

                @pl.when(mapped_lead)
                def _():
                    map_copy.start()
            upper = product.astype(bf16)
            high[k] = upper
            low[k] = (product - upper.astype(f32)).astype(bf16)

    extend_product(0, strips - 1)

    neighbours = sum(there.astype(jnp.int32) for there, _ in sides)
    pl.semaphore_wait(barrier, neighbours)

    @pl.when(not_right)
    def _():
        side[0][0].start()
        weights_right.start()

    @pl.when(not_left)
    def _():
        side[0][1].start()

    @pl.when(not_bottom)
    def _():
        first_down.start()

    @pl.when(not_top)
    def _():
        ups[0].start()

    extend_product(strips - 1, strips)

    for fetch in fetches[2:]:
        fetch.wait()
    own_cols = lax.broadcasted_iota(jnp.int32, (1, cols), 1) + me_c * cols
    pinned = jnp.zeros((1, cols), jnp.int32)
    for number in range(pins.shape[0]):
        pinned = pinned | (own_cols == pins[number]).astype(jnp.int32)
    pinned = jnp.broadcast_to(pinned, (rows, cols)) * (field_row == 0) * jnp.where(not_top, 0, 1)
    inertial = [
        inertia[...] * tgt[c] + jnp.where(pinned > 0, pin_stiffness * pos[c], 0.0)
        for c in range(3)
    ]

    wide = cols + 2 * LANES
    wide_lane = lax.broadcasted_iota(jnp.int32, (rows, wide), 1) - LANES
    wide_cols = wide_lane + me_c * cols
    grid_cols = n_col * cols
    vertical = jnp.where(field_row < rows - 1, stf[1], 0.0)
    is_last = field_row % srows == srows - 1
    w_down = jnp.where(is_last, vertical, 0.0)
    w_bottom = jnp.where(not_bottom, stf[1, rows - 1:rows], 0.0)
    rest_row = jnp.where(row_of == 1, 1.0, 0.0)

    def early_rhs(u, left, right, above, w_above):
        field = [jnp.concatenate([left[c], u[c], right[c]], axis=1) for c in range(3)]
        total = [jnp.zeros((rows, wide), f32)] * 3
        for number, offset in enumerate((1, 2)):
            ahead = [pltpu.roll(field[c], wide - offset, axis=1) for c in range(3)]
            gap = [ahead[c] - field[c] for c in range(3)]
            gap[0] = gap[0] + float(offset)
            scale = stretch(gap[0] * gap[0] + gap[1] * gap[1] + gap[2] * gap[2], float(offset))
            weight, cross = edge_w[number], cross_w[number]
            for c in range(3):
                moved = scale * gap[c]
                if c == 0:
                    moved = moved - float(offset)
                pull = weight * moved
                at_a = cross * ahead[c] - pull
                at_b = cross * field[c] + pull
                total[c] = total[c] + at_a + pltpu.roll(at_b, offset, axis=1)
        below = [pltpu.roll(u[c], rows - 1, axis=0) for c in range(3)]
        before = [
            jnp.where(field_row == 0, jnp.broadcast_to(above[c:c + 1], (rows, cols)),
                      pltpu.roll(u[c], 1, axis=0))
            for c in range(3)
        ]
        w_before = jnp.where(
            field_row == 0, jnp.broadcast_to(w_above, (rows, cols)),
            pltpu.roll(stf[1], 1, axis=0))
        gap = [below[c] - u[c] for c in range(3)]
        gap[1] = gap[1] + 1.0
        scale = stretch(gap[0] * gap[0] + gap[1] * gap[1] + gap[2] * gap[2], 1.0)
        back = [u[c] - before[c] for c in range(3)]
        back[1] = back[1] + 1.0
        back_scale = stretch(back[0] * back[0] + back[1] * back[1] + back[2] * back[2], 1.0)
        result = []
        for c in range(3):
            rest = 1.0 if c == 1 else 0.0
            value = inertial[c] + total[c][:, LANES:LANES + cols]
            value = value - vertical * (scale * gap[c] - rest) + w_down * below[c]
            result.append(value + w_before * (back_scale * back[c] - rest))
        return result

    def late_rhs(last_rows, below):
        gap = below - last_rows + rest_row
        scale = stretch(jnp.sum(gap * gap, axis=0, keepdims=True), 1.0)
        return w_bottom * (below - scale * gap + rest_row)

    def strip_vector(rhs, k):
        return [
            compact([rhs[c][srows * k + i:srows * k + i + 1] for c in range(3)])
            for i in range(srows)
        ]

    def receive(copy, there):
        @pl.when(there)
        def _():
            copy.wait_recv()

    def send(copy, there):
        @pl.when(there)
        def _():
            copy.start()

    @pl.when(not_left)
    def _():
        weights_right.wait_recv()

    for number, (offset, channel) in enumerate(((1, 0), (2, 2))):
        weight = jnp.concatenate(
            [halo_w[channel], stf[channel], jnp.zeros((rows, LANES), f32)], axis=1)
        inside = (wide_cols >= 0) & (wide_cols + offset <= grid_cols - 1)
        weight = jnp.where(inside, weight, 0.0)
        crossing = ((wide_lane < 0) & (wide_lane + offset >= 0)) | (
            (wide_lane < cols) & (wide_lane + offset >= cols))
        edge_w[number] = weight
        cross_w[number] = jnp.where(crossing, weight, 0.0)

    receive(first_down, not_top)
    above = recv_row[ITERS]
    w_above = jnp.where(not_top, above[3:4], 0.0)
    current = [pos[c] for c in range(3)]
    last_rows = compact([pos[c, rows - 1:rows] for c in range(3)])

    for sweep in range(ITERS):
        receive(side[sweep][0], not_left)
        receive(side[sweep][1], not_right)
        rhs = early_rhs(
            current, [halo[sweep, 0, c] for c in range(3)], [halo[sweep, 1, c] for c in range(3)],
            above, w_above)
        vectors = [strip_vector(rhs, k) for k in range(strips)]
        if sweep == 0:
            receive(ups[sweep], not_bottom)
            vectors[-1][-1] = vectors[-1][-1] + late_rhs(last_rows, recv_row[sweep])
        base, offsets = [], []
        for k in range(strips):
            parts = split(jnp.concatenate(vectors[k], axis=1))
            base.append(times_transposed(parts, mats[k]))
        carried = None
        for k in range(strips):
            if k == 0:
                carried = base[k][:, last_start:]
            else:
                carried = base[k][:, last_start:] + times_transposed(
                    split(carried), mats[k, last_start:, :cols])
            if k < strips - 1:
                carried = carried * w_strip[k]
            offsets.append(carried)
        def add_late():
            if sweep == 0:
                return 0.0
            ups[sweep].wait_recv()
            late = split(late_rhs(last_rows, recv_row[sweep]))
            change = times_transposed(late, mats[strips - 1, :, last_start:])
            late_change[...] = change
            return change[:, last_start:]

        @pl.when(is_lead & not_bottom)
        def _():
            send_row[base_row + sweep] = offsets[-1] + add_late()
            lead_out[sweep].start()

        def pass_on(tail_rows):
            send_row[base_row + ITERS + sweep] = tail_rows * w_bottom
            send_row[base_row + 2 * ITERS + sweep] = tail_rows
            send(next_out[sweep], is_tail & not_bottom)
            send(tail_out[sweep], tail_after)

        @pl.when(is_tail)
        def _():
            lead_out[sweep].wait_recv()
            lead_rows = recv_row[base_row + sweep]
            tail_rows = offsets[-1] + times_pair(
                split(lead_rows * w_above), high[strips - 1], low[strips - 1])

            @pl.when(jnp.logical_not(tail_before))
            def _():
                @pl.when(not_bottom)
                def _():
                    pass_on(tail_rows + add_late())

                above_row[...] = lead_rows

            @pl.when(tail_before)
            def _():
                if sweep == 0:
                    map_copy.wait_recv()
                    received = map_recv[...]
                    upper = received.astype(bf16)
                    map_high[...] = upper
                    map_low[...] = (received - upper.astype(f32)).astype(bf16)
                    both = times_pair(
                        split(received * w_above), high[strips - 1], low[strips - 1])
                    upper = both.astype(bf16)
                    both_high[...] = upper
                    both_low[...] = (both - upper.astype(f32)).astype(bf16)
                tail_out[sweep].wait_recv()
                entering = split(recv_row[base_row + ITERS + sweep])

                @pl.when(not_bottom)
                def _():
                    onward = tail_rows + times_pair(entering, both_high[...], both_low[...])
                    pass_on(onward + add_late())

                above_row[...] = lead_rows + times_pair(entering, map_high[...], map_low[...])

        @pl.when(lead_before)
        def _():
            next_out[sweep].wait_recv()
            above_row[...] = recv_row[base_row + 2 * ITERS + sweep]

        @pl.when(jnp.logical_not(not_top))
        def _():
            above_row[...] = jnp.zeros((SUB, cols), f32)

        if sweep > 0:
            base[-1] = base[-1] + late_change[...]
        above = above_row[...]
        entering = split(above * w_above)
        solved = [base[0] + times_transposed(entering, mats[0, :, :cols])]
        if sweep < ITERS - 1:
            send_row[sweep + 1] = solved[0][:, :cols]
            send(ups[sweep + 1], not_top)
        for k in range(1, strips):
            carried = offsets[k - 1] + times_pair(entering, high[k - 1], low[k - 1])
            solved.append(base[k] + times_transposed(split(carried), mats[k, :, :cols]))
        last_rows = solved[-1][:, last_start:]
        current = []
        for c in range(3):
            field = jnp.zeros((rows, cols), f32)
            for k in range(strips):
                for i in range(srows):
                    row = solved[k][c:c + 1, i * cols:(i + 1) * cols]
                    field = jnp.where(
                        field_row == srows * k + i, jnp.broadcast_to(row, (rows, cols)), field)
            current.append(field)
            if sweep < ITERS - 1:
                disp[c] = field
            else:
                out[c] = field
        if sweep < ITERS - 1:
            send(side[sweep + 1][0], not_right)
            send(side[sweep + 1][1], not_left)

    def sent(copy, there):
        @pl.when(there)
        def _():
            copy.wait_send()

    sent(weights_right, not_right)
    for right, left in side:
        sent(right, not_right)
        sent(left, not_left)
    for copy in ups:
        sent(copy, not_top)
    sent(first_down, not_bottom)
    sent(map_copy, mapped_lead)
    for t in range(ITERS):
        sent(lead_out[t], is_lead & not_bottom)
        sent(tail_out[t], tail_after)
        sent(next_out[t], is_tail & not_bottom)


def shards(n_strip, n_col, positions, target, inertia, stiffness, pin_columns, inverses):
    rows, cols = positions.shape[1:]
    strips, block, _ = inverses.shape
    messages = 4 * ITERS + 1
    dma = pltpu.SemaphoreType.DMA
    return pl.pallas_call(
        functools.partial(kernel, n_strip, n_col),
        out_shape=pltpu.VMEM(positions.shape, f32),
        in_specs=[pl.BlockSpec(memory_space=pltpu.HBM)] * 6,
        out_specs=pl.BlockSpec(memory_space=pltpu.VMEM),
        scratch_shapes=[
            pltpu.SMEM(pin_columns.shape, jnp.int32),
            pltpu.VMEM(positions.shape, f32),
            pltpu.VMEM(target.shape, f32),
            pltpu.VMEM(inertia.shape, f32),
            pltpu.VMEM(stiffness.shape, f32),
            pltpu.VMEM(inverses.shape, bf16),
            pltpu.VMEM((strips, cols, cols), bf16),
            pltpu.VMEM((strips, cols, cols), bf16),
            pltpu.VMEM(positions.shape, f32),
            pltpu.VMEM((ITERS, 2, 3, rows, LANES), f32),
            pltpu.VMEM((3, rows, LANES), f32),
            pltpu.VMEM((messages, SUB, cols), f32),
            pltpu.VMEM((messages, SUB, cols), f32),
            pltpu.VMEM((2, rows, cols + 2 * LANES), f32),
            pltpu.VMEM((2, rows, cols + 2 * LANES), f32),
            pltpu.VMEM((cols, cols), f32),
            pltpu.VMEM((cols, cols), f32),
            pltpu.VMEM((cols, cols), bf16),
            pltpu.VMEM((cols, cols), bf16),
            pltpu.VMEM((cols, cols), bf16),
            pltpu.VMEM((cols, cols), bf16),
            pltpu.VMEM((SUB, cols), f32),
            pltpu.VMEM((SUB, block), f32),
            dma((5,)),
            dma((strips,)),
            dma((ITERS, 2)),
            dma((ITERS, 2)),
            dma,
            dma,
            dma((messages,)),
            dma((messages,)),
            dma,
            dma,
        ],
        compiler_params=pltpu.CompilerParams(
            collective_id=0, has_side_effects=True, vmem_limit_bytes=67_000_000),
    )(pin_columns, positions, target, inertia, stiffness, inverses)


def solution(mesh):
    in_specs = (
        P(None, "strip", "col"),
        P(None, "strip", "col"),
        P("strip", "col"),
        P(None, "strip", "col"),
        P(),
        P("strip", None, None),
    )
    out_specs = P(None, "strip", "col")
    run = functools.partial(shards, mesh.shape["strip"], mesh.shape["col"])
    return jax.shard_map(run, mesh=mesh, in_specs=in_specs, out_specs=out_specs, check_vma=False)
```
